128 devices in a mesh: rep: 2 (over core), dp: 64 (over x, y, z).
Axes of the slice: x: 4, y: 4, z: 4, core: 2. Of those that a mesh axis runs over, the one named last changes fastest.
Arguments:
- x: bfloat16 [128, 1024, 1536], P(('rep', 'dp')), parts along dimension 0
- dy: bfloat16 [128, 1024, 1536], P(('rep', 'dp')), parts along dimension 0
- w_gate: bfloat16 [2, 1536, 4096], replicated
- w_up: bfloat16 [2, 1536, 4096], replicated
- w_down: bfloat16 [2, 4096, 1536], replicated
- m_w_gate: float32 [2, 1536, 4096], P(None, 'dp')
- m_w_up: float32 [2, 1536, 4096], P(None, 'dp')
- m_w_down: float32 [2, 4096, 1536], P(None, 'dp')
- v_w_gate: float32 [2, 1536, 4096], P(None, 'dp')
- v_w_up: float32 [2, 1536, 4096], P(None, 'dp')
- v_w_down: float32 [2, 4096, 1536], P(None, 'dp')
Outputs:
- output 1: bfloat16 [4, 1536, 4096], P('rep'), parts along dimension 0
- output 2: bfloat16 [4, 1536, 4096], P('rep'), parts along dimension 0
- output 3: bfloat16 [4, 4096, 1536], P('rep'), parts along dimension 0
- output 4: float32 [4, 1536, 4096], P('rep', 'dp'), parts along dimension 0
- output 5: float32 [4, 1536, 4096], P('rep', 'dp'), parts along dimension 0
- output 6: float32 [4, 4096, 1536], P('rep', 'dp'), parts along dimension 0
- output 7: float32 [4, 1536, 4096], P('rep', 'dp'), parts along dimension 0
- output 8: float32 [4, 1536, 4096], P('rep', 'dp'), parts along dimension 0
- output 9: float32 [4, 4096, 1536], P('rep', 'dp'), parts along dimension 0
There are 2 independent parts. The reference program is written for one: setup_inputs(seed, part) draws one part's arguments, and reference() takes and returns one part's arrays. A program takes and returns all parts, laid end to end along the dimension named above; an argument that names none is the same for every part.
All inputs are finite; a program needn't handle non-finite values.
Results may differ from the reference program's by a relative error of at most 0.022.
Values are sent between devices in bfloat16 or wider.
A program may use at most 1.5 GiB of HBM per device.

```python
import jax
import jax.numpy as jnp
from jax import lax

SEQUENCES = 64
TOKENS = 1024
D = 1536
FF = 4096
LAYERS = 2
NAMES = ("w_gate", "w_up", "w_down")
SHAPES = {"w_gate": (LAYERS, D, FF), "w_up": (LAYERS, D, FF), "w_down": (LAYERS, FF, D)}


def bump(key, n, height):
    away = (jnp.arange(n, dtype=jnp.int32) - jax.random.randint(key, (), 0, n, jnp.int32)) % n
    return jnp.where(away < n // 8, height, 1.0)


def together(key, own, strength):
    shared = jax.random.normal(key, own.shape[1:], jnp.float32)
    return (own + strength * shared) * lax.rsqrt(1 + strength * strength)


def setup_inputs(seed: int = 0, part: int = 0) -> dict:
    kx, kdy, ka, kb, kz, kf, kh, kl, *keys = jax.random.split(jax.random.key(seed), 8 + 3 * len(NAMES))
    kx, kdy, ka, kb = (jax.random.fold_in(k, part) for k in (kx, kdy, ka, kb))
    kw, km, kv = (keys[i::3] for i in range(3))
    shape = (SEQUENCES, TOKENS, D)
    much_x, much_dy = jax.random.uniform(kz, (2,), jnp.float32, 0.0, 1.0)
    loud = 2.0 ** jax.random.uniform(jax.random.fold_in(kz, 1), (), jnp.float32, -1.0, 2.0)
    layers = 2.0 ** jax.random.uniform(kl, (LAYERS, 1, 1), jnp.float32, -1.0, 1.0)
    x = together(ka, jax.random.normal(kx, shape, jnp.float32), much_x) * bump(kf, D, 4.0)
    dy = together(kb, jax.random.normal(kdy, shape, jnp.float32), much_dy)
    drawn = {"x": x.astype(jnp.bfloat16), "dy": (loud * dy * (SEQUENCES * TOKENS) ** -0.5).astype(jnp.bfloat16)}
    for key, name in zip(kw, NAMES, strict=True):
        w = jax.random.normal(key, SHAPES[name], jnp.float32) * SHAPES[name][1] ** -0.5
        drawn[name] = (w * {"w_gate": 1.0, "w_up": bump(kh, FF, 4.0), "w_down": layers}[name]).astype(jnp.bfloat16)
    for key, name in zip(km, NAMES, strict=True):
        drawn[f"m_{name}"] = 0.1 * jax.random.normal(key, SHAPES[name], jnp.float32)
    for key, name in zip(kv, NAMES, strict=True):
        drawn[f"v_{name}"] = loud * loud * jax.random.uniform(key, SHAPES[name], jnp.float32, 0.05, 0.15)
    return drawn


def matmul(a, w):
    return jnp.dot(a, w, preferred_element_type=jnp.float32).astype(jnp.bfloat16)


def normed(h):
    wide = h.astype(jnp.float32)
    scale = lax.rsqrt(jnp.mean(wide**2, -1, keepdims=True) + 1e-6)
    return (wide * scale).astype(jnp.bfloat16)


def layer(h, w):
    a = normed(h)
    gate = jnp.dot(a, w["w_gate"], preferred_element_type=jnp.float32)
    up = jnp.dot(a, w["w_up"], preferred_element_type=jnp.float32)
    return h + matmul((jax.nn.silu(gate) * up).astype(jnp.bfloat16), w["w_down"])


def adamw(w, m, v, g):
    m = 0.9 * m + 0.1 * g
    v = 0.95 * v + 0.05 * g * g
    step = m * lax.rsqrt(v + 1e-8) + 0.1 * w
    return (w - 0.02 * step).astype(jnp.bfloat16), m, v


def stack(weights, h):
    return lax.scan(lambda h, w: (layer(h, w), None), h, weights)[0]


def reference(x, dy, w_gate, w_up, w_down, m_w_gate, m_w_up, m_w_down, v_w_gate, v_w_up, v_w_down):
    weights = dict(zip(NAMES, (w_gate, w_up, w_down), strict=True))

    def take(so_far, sequence):
        h, by_y = sequence
        _, back = jax.vjp(lambda w: stack(w, h), weights)
        return jax.tree.map(lambda total, term: total + term.astype(jnp.float32), so_far, back(by_y)[0]), None

    none_yet = {name: jnp.zeros(w.shape, jnp.float32) for name, w in weights.items()}
    by_weights, _ = lax.scan(take, none_yet, (x, dy))
    gradients = [by_weights[name].astype(jnp.bfloat16).astype(jnp.float32) for name in NAMES]
    new = [
        adamw(w.astype(jnp.float32), m, v, g)
        for w, m, v, g in zip((w_gate, w_up, w_down), (m_w_gate, m_w_up, m_w_down), (v_w_gate, v_w_up, v_w_down), gradients, strict=True)
    ]
    return tuple(one[which] for which in range(3) for one in new)
```

```python
import functools
import jax, jax.numpy as jnp
from jax import lax
from jax.experimental import pallas as pl
from jax.experimental.pallas import tpu as pltpu
MESH = pl.DeviceIdType.MESH
BF, F32 = jnp.bfloat16, jnp.float32
ORDERS = ((0, 1, 2), (1, 2, 0), (2, 0, 1))
STRIDE = (16, 4, 1)

from jax.sharding import PartitionSpec as P

NAMES = ("w_gate", "w_up", "w_down")
KINDS = ("wide", "wide", "tall")


def place():
    me = lax.axis_index("dp")
    at = (me // 16, (me // 4) % 4, me % 4)
    def step(axis, by):
        return me + (lax.rem(at[axis] + by, 4) - at[axis]) * STRIDE[axis]
    right = [step(a, 1) for a in range(3)]
    left = [step(a, 3) for a in range(3)]
    return at, left, right

def greet(left, right):
    barrier = pltpu.get_barrier_semaphore()
    for to in (*left, *right):
        pl.semaphore_signal(barrier, inc=1, device_id={"dp": to}, device_id_type=MESH)
    pl.semaphore_wait(barrier, 6)

def piece(kind, color, half):
    if kind == "wide":
        cols = slice(None) if half is None else pl.ds(2048 * half, 2048)
        return (pl.ds(8 * color, 8), cols)
    cols = pl.ds(512 * color, 512) if half is None else pl.ds(512 * color + 256 * half, 256)
    return (slice(None), cols)

def gather_kernel(kinds, *refs):
    n = len(kinds)
    own, out = refs[:n], refs[n:2 * n]
    held, (lsem, psem, ssem, rsem) = refs[2 * n:3 * n], refs[3 * n:]
    at, left, right = place()
    loads = [pltpu.make_async_copy(own[m], held[m], lsem.at[m]) for m in range(n)]
    for c in loads: c.start()
    greet(left, right)
    mine = [pltpu.make_async_copy(held[m], out[m].at[at[0], at[1], at[2]], psem.at[m]) for m in range(n)]
    for m in range(n):
        loads[m].wait()
        mine[m].start()
    nxt = [lax.rem(a + 1, 4) for a in at]
    prv = [lax.rem(a + 3, 4) for a in at]

    def where(color, phase, j, half):
        order = ORDERS[color]
        idx = [at[0], at[1], at[2]]
        idx[order[phase]] = j
        for p in range(phase + 1, 3):
            idx[order[p]] = slice(None)
        return tuple(idx)

    def msg(m, color, phase, d, fwd, sending):
        axis = ORDERS[color][phase]
        a = at[axis]
        back, ahead = (prv[axis], nxt[axis]) if d == 0 else (nxt[axis], prv[axis])
        if sending:
            j = back if fwd else a
        else:
            j = lax.rem(a + 2, 4) if fwd else back
        half = d if fwd else None
        dst = out[m].at[(*where(color, phase, j, half), *piece(kinds[m], color, half))]
        src = dst
        if phase == 2 and not fwd:
            src = held[m].at[piece(kinds[m], color, None)]
        to = (right if d == 0 else left)[axis]
        k = (phase * 3 + color) * 4 + d * 2 + int(fwd)
        return pltpu.make_async_remote_copy(src_ref=src, dst_ref=dst, send_sem=ssem.at[m, k], recv_sem=rsem.at[m, k],
            device_id={"dp": to}, device_id_type=MESH)

    for phase in (2, 1, 0):
        for m in range(n):
            if phase == 1: mine[m].wait()
            for color in range(3):
                if phase < 2:
                    for d in (0, 1): msg(m, color, phase + 1, d, True, False).wait_recv()
                for d in (0, 1): msg(m, color, phase, d, False, True).start()
        for m in range(n):
            for color in range(3):
                for d in (0, 1):
                    msg(m, color, phase, d, False, False).wait_recv()
                    msg(m, color, phase, d, True, True).start()
    for m in range(n):
        for color in range(3):
            for d in (0, 1): msg(m, color, 0, d, True, False).wait_recv()
    for m in range(n):
        for phase in range(3):
            for color in range(3):
                for d in (0, 1):
                    for fwd in (False, True): msg(m, color, phase, d, fwd, True).wait_send()

BLOCK = {"wide": (24, 4096), "tall": (64, 1536)}

def gather(kinds, blocks, cid):
    n = len(kinds)
    return pl.pallas_call(
        functools.partial(gather_kernel, kinds),
        out_shape=[jax.ShapeDtypeStruct((4, 4, 4, *BLOCK[k]), BF) for k in kinds],
        in_specs=[pl.BlockSpec(memory_space=pl.ANY)] * n,
        out_specs=[pl.BlockSpec(memory_space=pl.ANY)] * n,
        scratch_shapes=[*(pltpu.VMEM(BLOCK[k], BF) for k in kinds),
            pltpu.SemaphoreType.DMA((n,)), pltpu.SemaphoreType.DMA((n,)),
            pltpu.SemaphoreType.DMA((n, 36)), pltpu.SemaphoreType.DMA((n, 36))],
        compiler_params=pltpu.CompilerParams(collective_id=cid, has_side_effects=True, vmem_limit_bytes=60 << 20),
        name="gather",
    )(*blocks)

PIECE = {"wide": (8, 2048), "tall": (64, 256)}
SLOTS = 4


def scatter_scratch(kinds):
    n, out = len(kinds), {}
    for m, kind in enumerate(kinds):
        p = PIECE[kind]
        for phase, lead in ((1, (3, 2, 4, 4)), (2, (3, 2, 4)), (3, (3, 2))):
            for letter in "ABC":
                out[f"{letter}{phase}", m] = pltpu.VMEM((*lead, *p), BF)
            if phase > 1:
                for letter in "AB":
                    out[f"{letter}s{phase}", m] = pltpu.VMEM((*lead, *p), BF)
                for letter in "CK":
                    out[f"{letter}o{phase}", m] = pltpu.VMEM((*lead, *p), F32)
        out["G", m] = pltpu.VMEM(BLOCK[kind], BF)
    for kind in dict.fromkeys(kinds):
        out["slot", kind] = pltpu.VMEM((SLOTS, 4, 4, *PIECE[kind]), BF)
        out["slot_sem", kind] = pltpu.SemaphoreType.DMA((SLOTS,))
    out["out_sem"] = pltpu.SemaphoreType.DMA((n,))
    out["send"] = pltpu.SemaphoreType.DMA((n, 54))
    out["recv"] = pltpu.SemaphoreType.DMA((n, 54))
    return out


class Scatter:
    def __init__(self, kinds, src, dst, has):
        self.kinds, self.src, self.dst, self.has = kinds, src, dst, has
        self.at, self.left, self.right = place()
        self.by = [[lax.rem(a + o, 4) for a in self.at] for o in range(4)]
        ms = range(len(kinds))
        self.loads = {k: [(m, u, c, d) for u in (0, 1) for m in ms if kinds[m] == k for c in range(3) for d in (0, 1)] for k in kinds}
        self.taken = {k: 0 for k in kinds}

    def ahead(self, d):
        return 1 if d == 0 else 3

    def load(self, kind, i):
        m, use, c, d = self.loads[kind][i]
        axis = ORDERS[c][0]
        idx = [slice(None)] * 3
        idx[axis] = self.by[0 if use else self.ahead(d)][axis]
        return pltpu.make_async_copy(self.src[m].at[(*idx, *piece(kind, c, d))], self.has["slot", kind].at[i % SLOTS],
            self.has["slot_sem", kind].at[i % SLOTS])

    def take(self, m, use, c, d):
        kind = self.kinds[m]
        i = self.taken[kind]
        assert self.loads[kind][i] == (m, use, c, d)
        self.load(kind, i).wait()
        return self.has["slot", kind].at[i % SLOTS]

    def give(self, m):
        kind = self.kinds[m]
        i = self.taken[kind]
        self.taken[kind] += 1
        if i + SLOTS < len(self.loads[kind]):
            self.load(kind, i + SLOTS).start()

    def copy(self, letter, phase, m, c, d):
        axis = ORDERS[c][phase - 1]
        if letter == "C":
            src = self.has[f"A{phase}", m].at[c, d]
        elif phase > 1:
            src = self.has[f"{letter}s{phase}", m].at[c, d]
        else:
            idx = [slice(None)] * 3
            idx[axis] = self.by[2 if letter == "A" else self.ahead(d)][axis]
            src = self.src[m].at[(*idx, *piece(self.kinds[m], c, d if letter == "A" else 1 - d))]
        k = ((phase - 1) * 3 + "ABC".index(letter)) * 6 + c * 2 + d
        return pltpu.make_async_remote_copy(src_ref=src, dst_ref=self.has[f"{letter}{phase}", m].at[c, d],
            send_sem=self.has["send"].at[m, k], recv_sem=self.has["recv"].at[m, k],
            device_id={"dp": (self.right if d == 0 else self.left)[axis]}, device_id_type=MESH)

    def begin(self):
        for kind in self.loads:
            for i in range(SLOTS):
                self.load(kind, i).start()

    def send(self, m):
        for letter in "AB":
            for c in range(3):
                for d in (0, 1):
                    self.copy(letter, 1, m, c, d).start()

    def combine(self, phase, m, c, d):
        self.copy("A", phase, m, c, d).wait_recv()
        a = self.has[f"A{phase}", m].at[c, d]
        if phase == 1:
            own = self.take(m, 0, c, d)

            @pl.loop(0, 16)
            def _(i):
                at = (i // 4, i % 4)
                a[at] = (a[at].astype(F32) + own[at].astype(F32)).astype(BF)

            self.give(m)
        elif phase == 2:
            own = self.has["Co2", m].at[c, d]

            @pl.loop(0, 4)
            def _(i):
                a[i] = (a[i].astype(F32) + own[i]).astype(BF)
        else:
            a[...] = (a[...].astype(F32) + self.has["Co3", m][c, d]).astype(BF)
        self.copy("C", phase, m, c, d).start()

    def roles(self, h):
        return (("As", h, 2), ("Bs", 1 - h, self.ahead(1 - h)), ("Co", h, self.ahead(h)), ("Ko", h, 0))

    def total(self, phase, m, c, h):
        self.copy("C", phase, m, c, h).wait_recv()
        self.copy("B", phase, m, c, 1 - h).wait_recv()
        one, two = self.has[f"C{phase}", m].at[c, h], self.has[f"B{phase}", m].at[c, 1 - h]
        order = ORDERS[c]
        if phase == 1:
            own = self.take(m, 1, c, h)
            for name, d, o in self.roles(h):
                to = self.has[f"{name}2", m].at[c, d]
                t = self.by[o][order[1]]

                @pl.loop(0, 4)
                def _(i):
                    at = (t, i) if order[1] < order[2] else (i, t)
                    to[i] = (own[at].astype(F32) + one[at].astype(F32) + two[at].astype(F32)).astype(to.dtype)

                if name in ("As", "Bs"):
                    self.copy(name[0], 2, m, c, d).start()
            self.give(m)
        elif phase == 2:
            own = self.has["Ko2", m].at[c, h]
            for name, d, o in self.roles(h):
                t = self.by[o][order[2]]
                to = self.has[f"{name}3", m].at[c, d]
                to[...] = (own[t] + one[t].astype(F32) + two[t].astype(F32)).astype(to.dtype)
                if name in ("As", "Bs"):
                    self.copy(name[0], 3, m, c, d).start()
        else:
            whole = self.has["Ko3", m][c, h] + one[...].astype(F32) + two[...].astype(F32)
            self.has["G", m][piece(self.kinds[m], c, h)] = whole.astype(BF)

    def out(self, m):
        return pltpu.make_async_copy(self.has["G", m], self.dst[m], self.has["out_sem"].at[m])

    def steps(self):
        ms = range(len(self.kinds))
        for phase in (1, 2, 3):
            for what in (self.combine, self.total):
                for m in ms:
                    for c in range(3):
                        for d in (0, 1):
                            yield functools.partial(what, phase, m, c, d)
        for m in ms:
            yield lambda m=m: self.out(m).start()

    def end(self):
        for m in range(len(self.kinds)):
            self.out(m).wait()
            for phase in (1, 2, 3):
                for letter in "ABC":
                    for c in range(3):
                        for d in (0, 1):
                            self.copy(letter, phase, m, c, d).wait_send()


def scatter_kernel(kinds, names, *refs):
    n = len(kinds)
    src, dst, has = refs[:n], refs[n:2 * n], dict(zip(names, refs[2 * n:], strict=True))
    it = Scatter(kinds, src, dst, has)
    it.begin()
    greet(it.left, it.right)
    for m in range(n):
        it.send(m)
    for step in it.steps():
        step()
    it.end()


def scatter(kinds, whole, cid):
    n = len(kinds)
    held = scatter_scratch(kinds)
    return pl.pallas_call(
        functools.partial(scatter_kernel, kinds, tuple(held)),
        out_shape=[jax.ShapeDtypeStruct(BLOCK[k], BF) for k in kinds],
        in_specs=[pl.BlockSpec(memory_space=pl.ANY)] * n,
        out_specs=[pl.BlockSpec(memory_space=pl.ANY)] * n,
        scratch_shapes=list(held.values()),
        compiler_params=pltpu.CompilerParams(collective_id=cid, has_side_effects=True, vmem_limit_bytes=63 << 20),
        name="scatter",
    )(*(w.reshape(4, 4, 4, *BLOCK[k]) for w, k in zip(whole, kinds)))


def matmul(a, w):
    return jnp.dot(a, w, preferred_element_type=F32).astype(BF)


def normed(h):
    wide = h.astype(F32)
    scale = lax.rsqrt(jnp.mean(wide**2, -1, keepdims=True) + 1e-6)
    return (wide * scale).astype(BF)


def layer(h, w):
    a = normed(h)
    gate = jnp.dot(a, w[0], preferred_element_type=F32)
    up = jnp.dot(a, w[1], preferred_element_type=F32)
    return h + matmul((jax.nn.silu(gate) * up).astype(BF), w[2])


def adamw(w, m, v, g):
    m = 0.9 * m + 0.1 * g
    v = 0.95 * v + 0.05 * g * g
    step = m * lax.rsqrt(v + 1e-8) + 0.1 * w
    return (w - 0.02 * step).astype(BF), m, v


def solution(mesh):
    def step(x, dy, *arrays):
        weights, m, v = (arrays[i : i + 3] for i in (0, 3, 6))
        me = lax.axis_index("dp")
        layers = weights[0].shape[0]
        h, backs = x[0], []
        for number in range(layers):
            h, back = jax.vjp(layer, h, tuple(w[number] for w in weights))
            backs.append(back)
        by_h, sums = dy[0], [None] * layers
        for number in reversed(range(layers)):
            by_h, by_w = backs[number](by_h)
            sums[number] = by_w
        for number in reversed(range(layers)):
            sums[number] = scatter(KINDS, sums[number], 1)
        new = []
        for i, kind in enumerate(KINDS):
            w = lax.dynamic_slice_in_dim(weights[i], me * BLOCK[kind][0], BLOCK[kind][0], axis=1)
            g = jnp.stack([sums[number][i] for number in range(layers)])
            new.append(adamw(w.astype(F32), m[i], v[i], g.astype(F32)))
        whole = gather(KINDS * layers, [new[i][0][number] for number in range(layers) for i in range(3)], 2)
        out = [jnp.stack([whole[number * 3 + i].reshape(weights[i].shape[1:]) for number in range(layers)]) for i in range(3)]
        return (*out, *(new[i][which] for which in (1, 2) for i in range(3)))

    blocks = P(None, "dp", None)
    return jax.shard_map(step, mesh=mesh, in_specs=(P(("rep", "dp")),) * 2 + (P(),) * 3 + (blocks,) * 6,
        out_specs=(P("rep"),) * 3 + (P("rep", "dp", None),) * 6, check_vma=False)
```

```python
import functools
import jax, jax.numpy as jnp
from jax import lax
from jax.experimental import pallas as pl
from jax.experimental.pallas import tpu as pltpu
MESH = pl.DeviceIdType.MESH
BF, F32 = jnp.bfloat16, jnp.float32
ORDERS = ((0, 1, 2), (1, 2, 0), (2, 0, 1))
STRIDE = (16, 4, 1)

from jax.sharding import PartitionSpec as P

NAMES = ("w_gate", "w_up", "w_down")
KINDS = ("wide", "wide", "tall")


def place():
    me = lax.axis_index("dp")
    at = (me // 16, (me // 4) % 4, me % 4)
    def step(axis, by):
        return me + (lax.rem(at[axis] + by, 4) - at[axis]) * STRIDE[axis]
    right = [step(a, 1) for a in range(3)]
    left = [step(a, 3) for a in range(3)]
    return at, left, right

def greet(left, right):
    barrier = pltpu.get_barrier_semaphore()
    for to in (*left, *right):
        pl.semaphore_signal(barrier, inc=1, device_id={"dp": to}, device_id_type=MESH)
    pl.semaphore_wait(barrier, 6)

def piece(kind, color, half):
    if kind == "wide":
        cols = slice(None) if half is None else pl.ds(2048 * half, 2048)
        return (pl.ds(8 * color, 8), cols)
    cols = pl.ds(512 * color, 512) if half is None else pl.ds(512 * color + 256 * half, 256)
    return (slice(None), cols)

def gather_kernel(kinds, *refs):
    n = len(kinds)
    own, out = refs[:n], refs[n:2 * n]
    held, (lsem, psem, ssem, rsem) = refs[2 * n:3 * n], refs[3 * n:]
    at, left, right = place()
    loads = [pltpu.make_async_copy(own[m], held[m], lsem.at[m]) for m in range(n)]
    for c in loads: c.start()
    greet(left, right)
    mine = [pltpu.make_async_copy(held[m], out[m].at[at[0], at[1], at[2]], psem.at[m]) for m in range(n)]
    for m in range(n):
        loads[m].wait()
        mine[m].start()
    nxt = [lax.rem(a + 1, 4) for a in at]
    prv = [lax.rem(a + 3, 4) for a in at]

    def where(color, phase, j, half):
        order = ORDERS[color]
        idx = [at[0], at[1], at[2]]
        idx[order[phase]] = j
        for p in range(phase + 1, 3):
            idx[order[p]] = slice(None)
        return tuple(idx)

    def msg(m, color, phase, d, fwd, sending):
        axis = ORDERS[color][phase]
        a = at[axis]
        back, ahead = (prv[axis], nxt[axis]) if d == 0 else (nxt[axis], prv[axis])
        if sending:
            j = back if fwd else a
        else:
            j = lax.rem(a + 2, 4) if fwd else back
        half = d if fwd else None
        dst = out[m].at[(*where(color, phase, j, half), *piece(kinds[m], color, half))]
        src = dst
        if phase == 2 and not fwd:
            src = held[m].at[piece(kinds[m], color, None)]
        to = (right if d == 0 else left)[axis]
        k = (phase * 3 + color) * 4 + d * 2 + int(fwd)
        return pltpu.make_async_remote_copy(src_ref=src, dst_ref=dst, send_sem=ssem.at[m, k], recv_sem=rsem.at[m, k],
            device_id={"dp": to}, device_id_type=MESH)

    for phase in (2, 1, 0):
        for m in range(n):
            if phase == 1: mine[m].wait()
            for color in range(3):
                if phase < 2:
                    for d in (0, 1): msg(m, color, phase + 1, d, True, False).wait_recv()
                for d in (0, 1): msg(m, color, phase, d, False, True).start()
        for m in range(n):
            for color in range(3):
                for d in (0, 1):
                    msg(m, color, phase, d, False, False).wait_recv()
                    msg(m, color, phase, d, True, True).start()
    for m in range(n):
        for color in range(3):
            for d in (0, 1): msg(m, color, 0, d, True, False).wait_recv()
    for m in range(n):
        for phase in range(3):
            for color in range(3):
                for d in (0, 1):
                    for fwd in (False, True): msg(m, color, phase, d, fwd, True).wait_send()

BLOCK = {"wide": (24, 4096), "tall": (64, 1536)}

def gather(kinds, blocks, cid):
    n = len(kinds)
    return pl.pallas_call(
        functools.partial(gather_kernel, kinds),
        out_shape=[jax.ShapeDtypeStruct((4, 4, 4, *BLOCK[k]), BF) for k in kinds],
        in_specs=[pl.BlockSpec(memory_space=pl.ANY)] * n,
        out_specs=[pl.BlockSpec(memory_space=pl.ANY)] * n,
        scratch_shapes=[*(pltpu.VMEM(BLOCK[k], BF) for k in kinds),
            pltpu.SemaphoreType.DMA((n,)), pltpu.SemaphoreType.DMA((n,)),
            pltpu.SemaphoreType.DMA((n, 36)), pltpu.SemaphoreType.DMA((n, 36))],
        compiler_params=pltpu.CompilerParams(collective_id=cid, has_side_effects=True, vmem_limit_bytes=VMEM),
        name="gather",
    )(*blocks)

PIECE = {"wide": (8, 2048), "tall": (64, 256)}
SLOTS = 4
VMEM = 67043328


def scatter_scratch(kinds, far=""):
    n, out, away = len(kinds), {}, {}
    for m, kind in enumerate(kinds):
        p = PIECE[kind]
        for phase, lead in ((1, (3, 2, 4, 4)), (2, (3, 2, 4)), (3, (3, 2))):
            for letter in "ABC":
                if phase == 1 and letter in far:
                    away[f"{letter}1", m] = jax.ShapeDtypeStruct((*lead, *p), BF)
                else:
                    out[f"{letter}{phase}", m] = pltpu.VMEM((*lead, *p), BF)
            if phase > 1:
                for letter in "AB":
                    out[f"{letter}s{phase}", m] = pltpu.VMEM((*lead, *p), BF)
                for letter in "CK":
                    out[f"{letter}o{phase}", m] = pltpu.VMEM((*lead, *p), F32)
        out["G", m] = pltpu.VMEM(BLOCK[kind], BF)
    for kind in dict.fromkeys(kinds):
        out["slot", kind] = pltpu.VMEM((SLOTS, 4, 4, *PIECE[kind]), BF)
        out["slot_sem", kind] = pltpu.SemaphoreType.DMA((SLOTS,))
        if far:
            out["land", kind] = pltpu.VMEM((2, 2, 4, 4, *PIECE[kind]), BF)
            out["land_sem", kind] = pltpu.SemaphoreType.DMA((2, 2))
    out["out_sem"] = pltpu.SemaphoreType.DMA((n,))
    out["send"] = pltpu.SemaphoreType.DMA((n, 54))
    out["recv"] = pltpu.SemaphoreType.DMA((n, 54))
    return out, away


class Scatter:
    def __init__(self, kinds, src, dst, has, far=""):
        self.kinds, self.src, self.dst, self.has, self.far = kinds, src, dst, has, far
        self.at, self.left, self.right = place()
        self.by = [[lax.rem(a + o, 4) for a in self.at] for o in range(4)]
        ms = range(len(kinds))
        self.loads = {k: [(m, u, c, d) for u in (0, 1) for m in ms if kinds[m] == k for c in range(3) for d in (0, 1)] for k in kinds}
        self.taken = {k: 0 for k in kinds}

    def ahead(self, d):
        return 1 if d == 0 else 3

    def load(self, kind, i):
        m, use, c, d = self.loads[kind][i]
        axis = ORDERS[c][0]
        idx = [slice(None)] * 3
        idx[axis] = self.by[0 if use else self.ahead(d)][axis]
        return pltpu.make_async_copy(self.src[m].at[(*idx, *piece(kind, c, d))], self.has["slot", kind].at[i % SLOTS],
            self.has["slot_sem", kind].at[i % SLOTS])

    def take(self, m, use, c, d):
        kind = self.kinds[m]
        i = self.taken[kind]
        assert self.loads[kind][i] == (m, use, c, d)
        self.load(kind, i).wait()
        return self.has["slot", kind].at[i % SLOTS]

    def give(self, m):
        kind = self.kinds[m]
        i = self.taken[kind]
        self.taken[kind] += 1
        if i + SLOTS < len(self.loads[kind]):
            self.load(kind, i + SLOTS).start()

    def copy(self, letter, phase, m, c, d):
        axis = ORDERS[c][phase - 1]
        if letter == "C":
            src = self.has[f"A{phase}", m].at[c, d]
        elif phase > 1:
            src = self.has[f"{letter}s{phase}", m].at[c, d]
        else:
            idx = [slice(None)] * 3
            idx[axis] = self.by[2 if letter == "A" else self.ahead(d)][axis]
            src = self.src[m].at[(*idx, *piece(self.kinds[m], c, d if letter == "A" else 1 - d))]
        k = ((phase - 1) * 3 + "ABC".index(letter)) * 6 + c * 2 + d
        return pltpu.make_async_remote_copy(src_ref=src, dst_ref=self.has[f"{letter}{phase}", m].at[c, d],
            send_sem=self.has["send"].at[m, k], recv_sem=self.has["recv"].at[m, k],
            device_id={"dp": (self.right if d == 0 else self.left)[axis]}, device_id_type=MESH)

    def begin(self):
        for kind in self.loads:
            for i in range(SLOTS):
                self.load(kind, i).start()

    def send(self, m):
        for letter in "AB":
            for c in range(3):
                for d in (0, 1):
                    self.copy(letter, 1, m, c, d).start()

    def combine(self, phase, m, c, d):
        self.copy("A", phase, m, c, d).wait_recv()
        a = self.has[f"A{phase}", m].at[c, d]
        if phase == 1:
            own = self.take(m, 0, c, d)

            @pl.loop(0, 16)
            def _(i):
                at = (i // 4, i % 4)
                a[at] = (a[at].astype(F32) + own[at].astype(F32)).astype(BF)

            self.give(m)
        elif phase == 2:
            own = self.has["Co2", m].at[c, d]

            @pl.loop(0, 4)
            def _(i):
                a[i] = (a[i].astype(F32) + own[i]).astype(BF)
        else:
            a[...] = (a[...].astype(F32) + self.has["Co3", m][c, d]).astype(BF)
        self.copy("C", phase, m, c, d).start()

    def roles(self, h):
        return (("As", h, 2), ("Bs", 1 - h, self.ahead(1 - h)), ("Co", h, self.ahead(h)), ("Ko", h, 0))

    def landed(self, m, c, h):
        kind = self.kinds[m]
        k = (c * 2 + h) % 2
        return [pltpu.make_async_copy(self.has[f"{letter}1", m].at[c, d], self.has["land", kind].at[k, i], self.has["land_sem", kind].at[k, i])
            for i, (letter, d) in enumerate((("C", h), ("B", 1 - h)))]

    def fetch(self, m, c, h):
        for letter, d, copy in zip("CB", (h, 1 - h), self.landed(m, c, h)):
            self.copy(letter, 1, m, c, d).wait_recv()
            copy.start()

    def total(self, phase, m, c, h):
        if phase == 1 and self.far:
            for copy in self.landed(m, c, h):
                copy.wait()
            one, two = (self.has["land", self.kinds[m]].at[(c * 2 + h) % 2, i] for i in (0, 1))
        else:
            self.copy("C", phase, m, c, h).wait_recv()
            self.copy("B", phase, m, c, 1 - h).wait_recv()
            one, two = self.has[f"C{phase}", m].at[c, h], self.has[f"B{phase}", m].at[c, 1 - h]
        order = ORDERS[c]
        if phase == 1:
            own = self.take(m, 1, c, h)
            for name, d, o in self.roles(h):
                to = self.has[f"{name}2", m].at[c, d]
                t = self.by[o][order[1]]

                @pl.loop(0, 4)
                def _(i):
                    at = (t, i) if order[1] < order[2] else (i, t)
                    to[i] = (own[at].astype(F32) + one[at].astype(F32) + two[at].astype(F32)).astype(to.dtype)

                if name in ("As", "Bs"):
                    self.copy(name[0], 2, m, c, d).start()
            self.give(m)
        elif phase == 2:
            own = self.has["Ko2", m].at[c, h]
            for name, d, o in self.roles(h):
                t = self.by[o][order[2]]
                to = self.has[f"{name}3", m].at[c, d]
                to[...] = (own[t] + one[t].astype(F32) + two[t].astype(F32)).astype(to.dtype)
                if name in ("As", "Bs"):
                    self.copy(name[0], 3, m, c, d).start()
        else:
            whole = self.has["Ko3", m][c, h] + one[...].astype(F32) + two[...].astype(F32)
            self.has["G", m][piece(self.kinds[m], c, h)] = whole.astype(BF)

    def out(self, m):
        return pltpu.make_async_copy(self.has["G", m], self.dst[m], self.has["out_sem"].at[m])

    def groups(self):
        ms, flows = range(len(self.kinds)), [(c, d) for c in range(3) for d in (0, 1)]
        out = []
        for phase in (1, 2, 3):
            for what in (self.combine, self.total):
                for m in ms:
                    group = [functools.partial(what, phase, m, *flow) for flow in flows]
                    if phase == 1 and what == self.total and self.far:
                        ahead = [functools.partial(self.fetch, m, *flow) for flow in flows]
                        group = ahead[:2] + [step for i in range(6) for step in (group[i], *ahead[i + 2:i + 3])]
                    out.append(group)
        return out + [[lambda m=m: self.out(m).start() for m in ms]]

    def end(self):
        for m in range(len(self.kinds)):
            self.out(m).wait()
            for phase in (1, 2, 3):
                for letter in "ABC":
                    for c in range(3):
                        for d in (0, 1):
                            self.copy(letter, phase, m, c, d).wait_send()


def scatter_kernel(kinds, names, *refs):
    n = len(kinds)
    src, dst, has = refs[:n], refs[n:2 * n], dict(zip(names, refs[2 * n:], strict=True))
    it = Scatter(kinds, src, dst, has)
    it.begin()
    greet(it.left, it.right)
    for m in range(n):
        it.send(m)
    for group in it.groups():
        for step in group:
            step()
    it.end()


def scatter(kinds, whole, cid):
    n = len(kinds)
    held, _ = scatter_scratch(kinds)
    return pl.pallas_call(
        functools.partial(scatter_kernel, kinds, tuple(held)),
        out_shape=[jax.ShapeDtypeStruct(BLOCK[k], BF) for k in kinds],
        in_specs=[pl.BlockSpec(memory_space=pl.ANY)] * n,
        out_specs=[pl.BlockSpec(memory_space=pl.ANY)] * n,
        scratch_shapes=list(held.values()),
        compiler_params=pltpu.CompilerParams(collective_id=cid, has_side_effects=True, vmem_limit_bytes=VMEM),
        name="scatter",
    )(*(w.reshape(4, 4, 4, *BLOCK[k]) for w, k in zip(whole, kinds)))


def dot(a, b, over=(1, 0)):
    return lax.dot_general(a, b, ((over[:1], over[1:]), ((), ())), preferred_element_type=F32)


WIDTH = 512
ROWS = 128
PLAN1 = (2, 4, 5, 6, 7)
PLAN0 = (2, 4, 6)
ONCE = pl.Buffered(1)
ANYWHERE = pl.BlockSpec(memory_space=pl.ANY)


def normed(h):
    wide = h.astype(F32)
    scale = lax.rsqrt(jnp.mean(wide**2, -1, keepdims=True) + 1e-6)
    return (wide * scale).astype(BF)


def normed_back(h, by_a, by_h):
    wide, by_a = h.astype(F32), by_a.astype(F32)
    scale = lax.rsqrt(jnp.mean(wide**2, -1, keepdims=True) + 1e-6)
    along = jnp.mean(by_a * wide, -1, keepdims=True)
    return (by_h.astype(F32) + (by_a * scale - wide * (along * scale**3)).astype(BF).astype(F32)).astype(BF)


def specs(tokens, d, layer):
    return (pl.BlockSpec((1, WIDTH, d), lambda i: (layer, i, 0)), pl.BlockSpec((1, d, WIDTH), lambda i: (layer, 0, i)),
        pl.BlockSpec((tokens, WIDTH), lambda i: (0, i)), pl.BlockSpec((WIDTH, d), lambda i: (i, 0)), pl.BlockSpec((d, WIDTH), lambda i: (0, i)),
        pl.BlockSpec((tokens, d), lambda i: (0, 0), pipeline_mode=ONCE))


def rows_of(ref):
    return [pl.ds(ROWS * r, ROWS) for r in range(ref.shape[0] // ROWS)]


def first_kernel(h, w_gate, w_up, w_down, gate, up, out, a, acc):
    tile = pl.program_id(0)

    @pl.when(tile == 0)
    def _():
        acc[...] = jnp.zeros_like(acc)
        for r in rows_of(h):
            a[r] = normed(h[r])

    g, u = dot(a[...], w_gate[0]), dot(a[...], w_up[0])
    gate[...], up[...] = g, u
    acc[...] += dot((jax.nn.silu(g) * u).astype(BF), w_down[0])

    @pl.when(tile == pl.num_programs(0) - 1)
    def _():
        for r in rows_of(h):
            out[r] = (h[r].astype(F32) + acc[r].astype(BF).astype(F32)).astype(BF)


def last_kernel(h, by_y, w_gate, w_up, gate, up, by_down, a_t, a):
    @pl.when(pl.program_id(0) == 0)
    def _():
        for r in rows_of(h):
            a[r] = normed(h[r])
            a_t[:, r] = a[r].T

    g, u = dot(a[...], w_gate[0]), dot(a[...], w_up[0])
    gate[...], up[...] = g, u
    by_down[...] = dot((jax.nn.silu(g) * u).astype(BF), by_y[...], (0, 0)).astype(BF)


def forward(h, by_y, weights, layer):
    (tokens, d), hidden = h.shape, weights[0].shape[2]
    w_down, w_in, across, by_w_down, _, states = specs(tokens, d, layer)
    flat, wide = jax.ShapeDtypeStruct((tokens, d), BF), jax.ShapeDtypeStruct((tokens, hidden), F32)
    call = functools.partial(pl.pallas_call, grid=(hidden // WIDTH,), compiler_params=pltpu.CompilerParams(vmem_limit_bytes=VMEM))
    if by_y is None:
        return call(first_kernel, in_specs=[states, w_in, w_in, w_down], out_specs=[across, across, states], out_shape=[wide, wide, flat],
            scratch_shapes=[pltpu.VMEM((tokens, d), BF), pltpu.VMEM((tokens, d), F32)], name="first")(h, *weights)
    turned = pl.BlockSpec((d, tokens), lambda i: (0, 0), pipeline_mode=ONCE)
    return call(last_kernel, in_specs=[states, states, w_in, w_in], out_specs=[across, across, by_w_down, turned],
        out_shape=[wide, wide, jax.ShapeDtypeStruct((hidden, d), BF), jax.ShapeDtypeStruct((d, tokens), BF)],
        scratch_shapes=[pltpu.VMEM((tokens, d), BF)], name="last")(h, by_y, *weights[:2])


def turn_back(refs, bufs, sems, by_h, a_t):
    rows = rows_of(by_h)

    def copies(r):
        return [pltpu.make_async_copy(ref.at[rows[r]], buf.at[r % 2], sems.at[r % 2, i]) for i, (ref, buf) in enumerate(zip(refs, bufs))]

    for copy in copies(0):
        copy.start()
    for r in range(len(rows)):
        if r + 1 < len(rows):
            for copy in copies(r + 1):
                copy.start()
        for copy in copies(r):
            copy.wait()
        h0, h1, by_y, by_a = (buf[r % 2] for buf in bufs)
        a_t[:, rows[r]] = normed(h0).T
        by_h[rows[r]] = normed_back(h1, by_a.astype(BF), by_y)


def backward_kernel(kinds, plan, names, top, *refs):
    refs = list(refs)
    pop = lambda n: [refs.pop(0) for _ in range(n)]
    n = len(kinds)
    src = pop(n)
    if top:
        by_h, a_t, gate, up, w_down, w_gate, w_up = pop(7)
    else:
        given, (gate, up, w_down) = pop(4), pop(3)
    dst, (by_gate_w, by_up_w, by_other) = pop(n), pop(3)
    away = pop(2 * n)
    if top:
        acc, acc_sem = pop(2)
    else:
        (by_h, a_t), bufs, (sems,) = pop(2), pop(4), pop(1)
    has = dict(zip(names, away + refs, strict=True))
    it = Scatter(kinds, src, dst, has, "BC")
    tile = pl.program_id(0)
    groups = it.groups()

    @pl.when(tile == 0)
    def _():
        it.begin()
        greet(it.left, it.right)
        for m in range(n):
            it.send(m)
        if top:
            acc[...] = jnp.zeros_like(acc)
        else:
            turn_back(given, bufs, sems, by_h, a_t)

    for number, group in zip(plan, groups):
        @pl.when(tile == number)
        def _():
            for step in group:
                step()

    g, u = gate[...], up[...]
    by_act = dot(by_h[...], w_down[0], (1, 1)).astype(BF).astype(F32)
    part = jax.nn.sigmoid(g)
    silu = g * part
    by_up = (by_act * silu).astype(BF)
    by_gate = (by_act * u * (part + silu * (1 - part))).astype(BF)
    by_gate_w[...] = dot(a_t[...], by_gate).astype(BF)
    by_up_w[...] = dot(a_t[...], by_up).astype(BF)
    if top:
        acc[...] += dot(by_gate, w_gate[0], (1, 1)) + dot(by_up, w_up[0], (1, 1))
    else:
        by_other[...] = dot((silu * u).astype(BF), by_h[...], (0, 0)).astype(BF)

    @pl.when(tile == pl.num_programs(0) - 1)
    def _():
        if top:
            pltpu.make_async_copy(acc, by_other, acc_sem).start()
        for group in groups[len(plan):]:
            for step in group:
                step()
        it.end()
        if top:
            pltpu.make_async_copy(acc, by_other, acc_sem).wait()


def backward(kinds, plan, whole, layer, states, gate, up, weights, cid):
    top, n = layer > 0, len(kinds)
    held, away = scatter_scratch(kinds, "BC")
    tokens, hidden = gate.shape
    d = weights[0].shape[1]
    w_down, w_in, across, by_w_down, by_w_in, flat = specs(tokens, d, layer)
    turned = pl.BlockSpec((d, tokens), lambda i: (0, 0), pipeline_mode=ONCE)
    args = [*(w.reshape(4, 4, 4, *BLOCK[k]) for w, k in zip(whole, kinds)), *states, gate, up, weights[2], *weights[:2 * top]]
    ins = [*[ANYWHERE] * n, *([flat, turned] if top else [ANYWHERE] * 4), across, across, w_down, *[w_in] * (2 * top)]
    outs = [*[ANYWHERE] * n, by_w_in, by_w_in, ANYWHERE if top else by_w_down, *[ANYWHERE] * len(away)]
    shapes = [*(jax.ShapeDtypeStruct(BLOCK[k], BF) for k in kinds), *[jax.ShapeDtypeStruct((d, hidden), BF)] * 2,
        jax.ShapeDtypeStruct((tokens, d), F32) if top else jax.ShapeDtypeStruct((hidden, d), BF), *away.values()]
    if top:
        scratch = [pltpu.VMEM((tokens, d), F32), pltpu.SemaphoreType.DMA]
    else:
        scratch = [pltpu.VMEM((tokens, d), BF), pltpu.VMEM((d, tokens), BF), *[pltpu.VMEM((2, ROWS, d), BF)] * 3, pltpu.VMEM((2, ROWS, d), F32),
            pltpu.SemaphoreType.DMA((2, 4))]
    return pl.pallas_call(
        functools.partial(backward_kernel, kinds, plan, (*away, *held), top),
        grid=(hidden // WIDTH,), in_specs=ins, out_specs=outs, out_shape=shapes, scratch_shapes=scratch + list(held.values()),
        compiler_params=pltpu.CompilerParams(collective_id=cid, has_side_effects=True, vmem_limit_bytes=VMEM),
        name="backward",
    )(*args)[:n + 3]


def adamw(w, m, v, g):
    m = 0.9 * m + 0.1 * g
    v = 0.95 * v + 0.05 * g * g
    step = m * lax.rsqrt(v + 1e-8) + 0.1 * w
    return (w - 0.02 * step).astype(BF), m, v


def solution(mesh):
    def step(x, dy, *arrays):
        weights, m, v = (arrays[i : i + 3] for i in (0, 3, 6))
        me = lax.axis_index("dp")
        layers = weights[0].shape[0]
        assert layers == 2
        h0, by_y = x[0], dy[0]
        gate0, up0, h1 = forward(h0, None, weights, 0)
        gate1, up1, by_down1, a_t = forward(h1, by_y, weights, 1)
        down1, by_gate1, by_up1, by_a1 = backward(("tall",), PLAN1, [by_down1], 1, [by_y, a_t], gate1, up1, weights, 3)
        top1, top2, *by0 = backward(("wide", "wide"), PLAN0, [by_gate1, by_up1], 0, [h0, h1, by_y, by_a1], gate0, up0, weights, 4)
        sums = [scatter(KINDS, by0, 1), [top1, top2, down1]]
        new = []
        for i, kind in enumerate(KINDS):
            w = lax.dynamic_slice_in_dim(weights[i], me * BLOCK[kind][0], BLOCK[kind][0], axis=1)
            g = jnp.stack([sums[number][i] for number in range(layers)])
            new.append(adamw(w.astype(F32), m[i], v[i], g.astype(F32)))
        whole = gather(KINDS * layers, [new[i][0][number] for number in range(layers) for i in range(3)], 2)
        out = [jnp.stack([whole[number * 3 + i].reshape(weights[i].shape[1:]) for number in range(layers)]) for i in range(3)]
        return (*out, *(new[i][which] for which in (1, 2) for i in range(3)))

    blocks = P(None, "dp", None)
    return jax.shard_map(step, mesh=mesh, in_specs=(P(("rep", "dp")),) * 2 + (P(),) * 3 + (blocks,) * 6,
        out_specs=(P("rep"),) * 3 + (P("rep", "dp", None),) * 6, check_vma=False)
```

```python
import functools
import jax, jax.numpy as jnp
from jax import lax
from jax.experimental import pallas as pl
from jax.experimental.pallas import tpu as pltpu
MESH = pl.DeviceIdType.MESH
BF, F32 = jnp.bfloat16, jnp.float32
ORDERS = ((0, 1, 2), (1, 2, 0), (2, 0, 1))
STRIDE = (16, 4, 1)

from jax.sharding import PartitionSpec as P

NAMES = ("w_gate", "w_up", "w_down")
KINDS = ("wide", "wide", "tall")


def place():
    me = lax.axis_index("dp")
    at = (me // 16, (me // 4) % 4, me % 4)
    def step(axis, by):
        return me + (lax.rem(at[axis] + by, 4) - at[axis]) * STRIDE[axis]
    right = [step(a, 1) for a in range(3)]
    left = [step(a, 3) for a in range(3)]
    return at, left, right

def greet(left, right):
    barrier = pltpu.get_barrier_semaphore()
    for to in (*left, *right):
        pl.semaphore_signal(barrier, inc=1, device_id={"dp": to}, device_id_type=MESH)
    pl.semaphore_wait(barrier, 6)

def piece(kind, color, half):
    if kind == "wide":
        return (color, slice(None), slice(None) if half is None else pl.ds(2048 * half, 2048))
    return (slice(None), slice(None), pl.ds(512 * color, 512) if half is None else pl.ds(512 * color + 256 * half, 256))

BLOCK = {"wide": (3, 8, 4096), "tall": (8, 8, 1536)}
PIECE = (8, 2048)


def over(n):
    def run(body):
        lax.fori_loop(0, n, lambda i, _: body(i), None)

    return run


WIDE = BLOCK["wide"]
VMEM = 67043328


def sums_scratch(n):
    near, away = {}, {}
    for m in range(n):
        for phase, lead in ((1, (3, 2, 4, 4)), (2, (3, 2, 4)), (3, (3, 2))):
            for letter in "ABC":
                if phase == 1:
                    away[f"{letter}1", m] = jax.ShapeDtypeStruct((*lead, *PIECE), BF)
                else:
                    near[f"{letter}{phase}", m] = pltpu.VMEM((*lead, *PIECE), BF)
    near["pass1"] = pltpu.VMEM((3, 2, 4, 4, *PIECE), BF)
    for phase, lead in ((2, (3, 2, 4)), (3, (3, 2))):
        near[f"send{phase}"] = pltpu.VMEM((2, *lead, *PIECE), BF)
        near[f"keep{phase}"] = pltpu.VMEM((2, *lead, *PIECE), F32)
    near["G"] = pltpu.VMEM((n, 3, 2, *PIECE), BF)
    near["land"] = pltpu.VMEM((2, 3, 2, 4, 4, *PIECE), BF)
    dma = pltpu.SemaphoreType.DMA
    near |= {"land_sem": dma((2,)), "sent": dma((n, 9)), "came1": dma((n, 3, 3)), "came": dma((n, 6))}
    return near, away


class Sums:
    def __init__(self, src, has):
        self.src, self.has = src, has
        self.at, self.left, self.right = place()
        self.by = [[lax.rem(a + o, 4) for a in self.at] for o in range(4)]

    def own(self, m, c, o, half):
        idx = [slice(None)] * 3
        idx[ORDERS[c][0]] = self.by[o][ORDERS[c][0]]
        return self.src[m].at[(*idx, *piece("wide", c, half))]

    def copy(self, letter, phase, m, c, d):
        k = "ABC".index(letter)
        to = self.has[f"{letter}{phase}", m]
        if c is None:
            src = dst = to
        elif d is None:
            src = dst = to.at[c]
        else:
            dst = to.at[c, d]
            if letter == "C":
                src = self.has["pass1"].at[c, d] if phase == 1 else self.has[f"A{phase}", m].at[c, d]
            elif phase > 1:
                src = self.has[f"send{phase}"].at[k, c, d]
            else:
                src = self.own(m, c, *((2, d) if letter == "A" else (1 + 2 * d, 1 - d)))
        came = self.has["came1"].at[m, k, c or 0] if phase == 1 else self.has["came"].at[m, phase * 3 - 6 + k]
        return pltpu.make_async_remote_copy(src_ref=src, dst_ref=dst, send_sem=self.has["sent"].at[m, phase * 3 - 3 + k], recv_sem=came,
            device_id={"dp": (self.left if d else self.right)[ORDERS[c or 0][phase - 1]]}, device_id_type=MESH)

    def send(self, letter, m, phase=1, colors=(0, 1, 2)):
        for c in colors:
            for d in (0, 1):
                self.copy(letter, phase, m, c, d).start()

    def came(self, letters, phase, m):
        for letter in letters:
            self.copy(letter, phase, m, None, None).wait_recv()

    def sent(self, letters, phase, m):
        for letter in letters:
            self.copy(letter, phase, m, None, None).wait_send()

    def fetch(self, what, m, c, slot):
        land, sem = self.has["land"].at[slot], self.has["land_sem"].at[slot]
        for i, letter in ((0, "A"),) if what == "c" else ((0, "C"), (2, "B")):
            self.copy(letter, 1, m, c, None).wait_recv()
            pltpu.make_async_copy(self.has[f"{letter}1", m].at[c], land.at[i], sem).start()
        for d in (0, 1):
            pltpu.make_async_copy(self.own(m, c, 1 + 2 * d if what == "c" else 0, d), land.at[1, d], sem).start()

    def first(self, what, m, c, slot):
        land = self.has["land"].at[slot]
        got = land.at[0:2] if what == "c" else land
        pltpu.make_async_copy(got, got, self.has["land_sem"].at[slot]).wait()
        if what == "c":
            if m > 0 and c == 0:
                self.sent("C", 1, m - 1)
            to = self.has["pass1"]

            @over(2)
            def _(d):
                @over(4)
                def _(i):
                    @over(4)
                    def _(j):
                        to[c, d, i, j] = (land[0, d, i, j].astype(F32) + land[1, d, i, j].astype(F32)).astype(BF)

            self.send("C", m, 1, (c,))
            return
        if m > 0 and c == 0:
            self.sent("AB", 2, m - 1)
        axis = ORDERS[c][1]

        def whole(h, t, i):
            at = (t, i) if axis < ORDERS[c][2] else (i, t)
            return land[(1, h, *at)].astype(F32) + land[(0, h, *at)].astype(F32) + land[(2, 1 - h, *at)].astype(F32)

        @over(2)
        def _(h):
            @over(2)
            def _(k):
                d, t, u = self.role(axis, h, k)

                @over(4)
                def _(i):
                    self.has["send2"][k, c, d, i] = whole(h, t, i).astype(BF)
                    self.has["keep2"][k, c, h, i] = whole(h, u, i)

        self.send("A", m, 2, (c,))
        self.send("B", m, 2, (c,))

    def role(self, axis, h, k):
        turn = k * (1 - 2 * h)
        return h + turn, lax.rem(self.at[axis] + 2 + turn, 4), lax.rem(self.at[axis] + k * (1 + 2 * h), 4)

    def later(self, what, phase, m):
        a, b, c_ = (self.has[f"{letter}{phase}", m] for letter in "ABC")
        keep = self.has[f"keep{phase}"]
        if what == "c":
            self.came("A", phase, m)

            @over(3)
            def _(c):
                @over(2)
                def _(d):
                    if phase == 3:
                        a[c, d] = (a[c, d].astype(F32) + keep[1, c, d]).astype(BF)
                    else:
                        @over(4)
                        def _(i):
                            a[c, d, i] = (a[c, d, i].astype(F32) + keep[1, c, d, i]).astype(BF)

            self.send("C", m, phase)
            return
        self.came("CB", phase, m)
        if phase == 3:
            @over(3)
            def _(c):
                @over(2)
                def _(h):
                    self.has["G"][m, c, h] = (keep[0, c, h] + c_[c, h].astype(F32) + b[c, 1 - h].astype(F32)).astype(BF)

            return
        if m > 0:
            self.sent("AB", 3, m - 1)
        for c in range(3):
            def whole(h, t):
                return keep[0, c, h, t] + c_[c, h, t].astype(F32) + b[c, 1 - h, t].astype(F32)

            @over(2)
            def _(h):
                @over(2)
                def _(k):
                    d, t, u = self.role(ORDERS[c][2], h, k)
                    self.has["send3"][k, c, d] = whole(h, t).astype(BF)
                    self.has["keep3"][k, c, h] = whole(h, u)

        self.send("A", m, 3)
        self.send("B", m, 3)

    def end(self, first, last):
        for m in range(first, last + 1):
            self.sent("AB" + "C" * (m == last), 1, m)
            for phase in (2, 3):
                self.sent("C" + "AB" * (m == last), phase, m)


ORDER = ((1, 2), (1, 0), (1, 1), (0, 2), (0, 0), (0, 1))
KIND_OF = tuple(KINDS[i] for _, i in ORDER)
SLOT_OF = tuple(KIND_OF[:m].count(k) for m, k in enumerate(KIND_OF))


def gather_scratch():
    out = {}
    for kind in dict.fromkeys(KIND_OF):
        n = KIND_OF.count(kind)
        out["moments", kind] = pltpu.VMEM((n, 2, *BLOCK[kind]), F32)
        out["w", kind] = pltpu.VMEM((n, *BLOCK[kind]), BF)
    return out


class Gather:
    def __init__(self, it, weights, moments, whole, new, has, sems):
        self.it, self.weights, self.moments, self.whole, self.new, self.has = it, weights, moments, whole, new, has
        self.load_sem, self.save_sem, self.mine_sem, self.ssem, self.rsem = sems

    def held(self, m):
        return self.has["w", KIND_OF[m]].at[SLOT_OF[m]]

    def loads(self, m):
        layer, i = ORDER[m]
        me = lax.axis_index("dp")
        refs = [self.weights[i].at[layer, me], *(ref.at[layer] for ref in self.moments[i])]
        bufs = [self.held(m), *(self.has["moments", KIND_OF[m]].at[SLOT_OF[m], j] for j in (0, 1))]
        return [pltpu.make_async_copy(ref, buf, self.load_sem.at[m, j]) for j, (ref, buf) in enumerate(zip(refs, bufs))]

    def saves(self, m):
        layer, i = ORDER[m]
        return [pltpu.make_async_copy(self.has["moments", KIND_OF[m]].at[SLOT_OF[m], j], self.new[i][j].at[layer], self.save_sem.at[m, j])
            for j in (0, 1)]

    def mine(self, m):
        at = self.it.at
        return pltpu.make_async_copy(self.held(m), self.whole[m].at[at[0], at[1], at[2]], self.mine_sem.at[m])

    def adamw(self, m):
        for copy in self.loads(m):
            copy.wait()
        w, moments, g = self.held(m), self.has["moments", KIND_OF[m]].at[SLOT_OF[m]], self.it.has["G"].at[m]

        @over(3)
        def _(c):
            @over(2)
            def _(h):
                @over(4)
                def _(i):
                    from_g = (c, h, slice(None), pl.ds(pl.multiple_of(512 * i, 512), 512))
                    if KIND_OF[m] == "wide":
                        at = (c, slice(None), pl.ds(pl.multiple_of(2048 * h + 512 * i, 512), 512))
                    else:
                        at = (4 * h + i, slice(None), pl.ds(pl.multiple_of(512 * c, 512), 512))
                    w[at], moments[(0, *at)], moments[(1, *at)] = adamw(w[at].astype(F32), moments[(0, *at)], moments[(1, *at)], g[from_g].astype(F32))

        self.mine(m).start()
        for copy in self.saves(m):
            copy.start()

    def msg(self, m, color, phase, d, fwd):
        order, at = ORDERS[color], self.it.at
        axis = order[phase]
        idx = list(at)
        if fwd:
            idx[axis] = self.it.by[3 if d == 0 else 1][axis]
        for p in range(phase + 1, 3):
            idx[order[p]] = slice(None)
        part = piece(KIND_OF[m], color, d if fwd else None)
        dst = self.whole[m].at[(*idx, *part)]
        src = self.held(m).at[part] if phase == 2 and not fwd else dst
        return self.sets(m, phase, fwd, src, dst, (self.it.right if d == 0 else self.it.left)[axis])

    def sets(self, m, phase, fwd, src, dst, to):
        k = phase * 2 + int(fwd)
        return pltpu.make_async_remote_copy(src_ref=src, dst_ref=dst, send_sem=self.ssem.at[m, k], recv_sem=self.rsem.at[m, k],
            device_id={"dp": to}, device_id_type=MESH)

    def all(self, m, phase, fwd):
        much = self.whole[m].at[(*(0,) * phase, slice(0, 1 if fwd else 2))]
        return self.sets(m, phase, fwd, much, much, self.it.right[0])

    def send(self, m, phase, fwd):
        if fwd:
            self.all(m, phase, False).wait_recv()
        elif phase < 2:
            self.all(m, phase + 1, True).wait_recv()
        if not fwd and phase == 1:
            self.mine(m).wait()
        for color in range(3):
            for d in (0, 1):
                self.msg(m, color, phase, d, fwd).start()

    def end(self):
        for m in range(len(ORDER)):
            for copy in self.saves(m):
                copy.wait()
            self.all(m, 0, True).wait_recv()
            for phase in range(3):
                for fwd in (False, True):
                    self.all(m, phase, fwd).wait_send()


def dot(a, b, over=(1, 0)):
    return lax.dot_general(a, b, ((over[:1], over[1:]), ((), ())), preferred_element_type=F32)


WIDTH = 512
ROWS = 128
ONCE = pl.Buffered(1)
ANYWHERE = pl.BlockSpec(memory_space=pl.ANY)


def normed(h):
    wide = h.astype(F32)
    scale = lax.rsqrt(jnp.mean(wide**2, -1, keepdims=True) + 1e-6)
    return (wide * scale).astype(BF)


def normed_back(h, by_a, by_h):
    wide, by_a = h.astype(F32), by_a.astype(F32)
    scale = lax.rsqrt(jnp.mean(wide**2, -1, keepdims=True) + 1e-6)
    along = jnp.mean(by_a * wide, -1, keepdims=True)
    return (by_h.astype(F32) + (by_a * scale - wide * (along * scale**3)).astype(BF).astype(F32)).astype(BF)


PACKED = pl.BlockSpec((WIDTH // 64, *WIDE), lambda i: (i, 0, 0, 0))


def specs(tokens, d, layer):
    return (pl.BlockSpec((1, WIDTH, d), lambda i: (layer, i, 0)), pl.BlockSpec((1, d, WIDTH), lambda i: (layer, 0, i)),
        pl.BlockSpec((tokens, WIDTH), lambda i: (0, i)), pl.BlockSpec((tokens, d), lambda i: (0, 0), pipeline_mode=ONCE))


def pack(out, tile):
    tile = tile.reshape(*out.shape[:-3], 8, 8, 1536)
    for c in range(3):
        for g in range(8):
            out[..., c, :, 512 * g:512 * g + 512] = tile[..., g, :, 512 * c:512 * c + 512].astype(BF)


def rows_of(ref):
    return [pl.ds(ROWS * r, ROWS) for r in range(ref.shape[0] // ROWS)]


def first_kernel(h, w_gate, w_up, w_down, gate, up, act, out, a, acc):
    tile = pl.program_id(0)

    @pl.when(tile == 0)
    def _():
        acc[...] = jnp.zeros_like(acc)
        for r in rows_of(h):
            a[r] = normed(h[r])

    g, u = dot(a[...], w_gate[0]), dot(a[...], w_up[0])
    gate[...], up[...] = g, u
    act[...] = (jax.nn.silu(g) * u).astype(BF)
    acc[...] += dot(act[...], w_down[0])

    @pl.when(tile == pl.num_programs(0) - 1)
    def _():
        for r in rows_of(h):
            out[r] = (h[r].astype(F32) + acc[r].astype(BF).astype(F32)).astype(BF)


def last_kernel(h, by_y, w_gate, w_up, gate, up, by_down, a_t, a):
    @pl.when(pl.program_id(0) == 0)
    def _():
        for r in rows_of(h):
            a[r] = normed(h[r])
            a_t[:, r] = a[r].T

    g, u = dot(a[...], w_gate[0]), dot(a[...], w_up[0])
    gate[...], up[...] = g, u
    pack(by_down, dot((jax.nn.silu(g) * u).astype(BF), by_y[...], (0, 0)))


def forward(h, by_y, weights, layer):
    (tokens, d), hidden = h.shape, weights[0].shape[2]
    w_down, w_in, across, states = specs(tokens, d, layer)
    flat, wide = jax.ShapeDtypeStruct((tokens, d), BF), jax.ShapeDtypeStruct((tokens, hidden), F32)
    call = functools.partial(pl.pallas_call, grid=(hidden // WIDTH,), compiler_params=pltpu.CompilerParams(vmem_limit_bytes=VMEM))
    if by_y is None:
        return call(first_kernel, in_specs=[states, w_in, w_in, w_down], out_specs=[across, across, across, states], out_shape=[wide, wide, jax.ShapeDtypeStruct(wide.shape, BF), flat],
            scratch_shapes=[pltpu.VMEM((tokens, d), BF), pltpu.VMEM((tokens, d), F32)], name="first")(h, *weights)
    turned = pl.BlockSpec((d, tokens), lambda i: (0, 0), pipeline_mode=ONCE)
    return call(last_kernel, in_specs=[states, states, w_in, w_in], out_specs=[across, across, PACKED, turned],
        out_shape=[wide, wide, jax.ShapeDtypeStruct((64, *WIDE), BF), jax.ShapeDtypeStruct((d, tokens), BF)],
        scratch_shapes=[pltpu.VMEM((tokens, d), BF)], name="last")(h, by_y, *weights[:2])


def adamw(w, m, v, g):
    m = 0.9 * m + 0.1 * g
    v = 0.95 * v + 0.05 * g * g
    step = m * lax.rsqrt(v + 1e-8) + 0.1 * w
    return (w - 0.02 * step).astype(BF), m, v


PLAN = {
    "start": {
        (0, 0): (('A', 0),),
    },
    "top": {
        (1, 0): (('B', 0),),
        (3, 1): (('F', 'c', 0, 0, 0), ('F', 'c', 0, 1, 1),),
        (4, 0): (('P', 'c', 0, 0, 0), ('F', 'c', 0, 2, 0),),
        (4, 1): (('P', 'c', 0, 1, 1),),
        (5, 0): (('P', 'c', 0, 2, 0),),
    },
    "up": {
        (0, 0): (('F', 't', 0, 0, 1), ('F', 't', 0, 1, 0), ('A', 1),),
        (1, 0): (('P', 't', 0, 0, 1), ('F', 't', 0, 2, 1), ('B', 1),),
        (2, 0): (('P', 't', 0, 1, 0),),
        (3, 0): (('P', 't', 0, 2, 1),),
        (6, 0): (('F', 'c', 1, 0, 0), ('F', 'c', 1, 1, 1),),
        (7, 0): (('P', 'c', 1, 0, 0), ('F', 'c', 1, 2, 0),),
    },
    "mid": {
        (0, 0): (('P', 'c', 1, 1, 1), ('A', 2),),
        (1, 0): (('P', 'c', 1, 2, 0), ('O', 'c', 2, 0),),
        (5, 0): (('F', 't', 1, 0, 1), ('F', 't', 1, 1, 0), ('B', 2),),
    },
    "turn": {
        (0, 0): (('O', 't', 2, 0),),
        (1, 0): (('P', 't', 1, 0, 1), ('F', 't', 1, 2, 1),),
        (2, 0): (('P', 't', 1, 1, 0), ('F', 'c', 2, 0, 0),),
        (3, 0): (('P', 't', 1, 2, 1), ('F', 'c', 2, 1, 1),),
    },
    "down": {
        (0, 0): (('O', 'c', 3, 0), ('P', 'c', 2, 0, 0), ('F', 'c', 2, 2, 0),),
        (1, 0): (('O', 'c', 2, 1), ('P', 'c', 2, 1, 1),),
        (2, 0): (('O', 't', 3, 0), ('P', 'c', 2, 2, 0),),
        (6, 0): (('F', 't', 2, 0, 1),),
    },
    "low": {
        (0, 0): (('O', 't', 2, 1), ('F', 't', 2, 1, 0), ('A', 3),),
        (0, 1): (('P', 't', 2, 0, 1), ('F', 't', 2, 2, 1), ('B', 3),),
        (1, 0): (('O', 'c', 3, 1), ('P', 't', 2, 1, 0),),
        (1, 1): (('P', 't', 2, 2, 1),),
        (3, 0): (('F', 'c', 3, 0, 0), ('F', 'c', 3, 1, 1),),
        (3, 1): (('P', 'c', 3, 0, 0), ('F', 'c', 3, 2, 0),),
        (4, 0): (('P', 'c', 3, 1, 1),),
        (4, 1): (('P', 'c', 3, 2, 0),),
        (5, 1): (('O', 'c', 2, 2),),
        (6, 1): (('O', 't', 3, 1),),
    },
    "last": {
        (0, 0): (('F', 't', 3, 0, 1), ('F', 't', 3, 1, 0), ('A', 4),),
        (1, 0): (('O', 't', 2, 2),),
        (2, 0): (('P', 't', 3, 0, 1), ('F', 't', 3, 2, 1), ('B', 4),),
        (3, 0): (('P', 't', 3, 1, 0),),
        (4, 0): (('P', 't', 3, 2, 1),),
        (6, 0): (('O', 'c', 3, 2), ('F', 'c', 4, 0, 0), ('F', 'c', 4, 1, 1),),
        (7, 0): (('P', 'c', 4, 0, 0), ('F', 'c', 4, 2, 0),),
    },
}
TAIL = (
    ('P', 'c', 4, 1, 1), ('P', 'c', 4, 2, 0), ('u', 0), ('u', 1), ('g', 0, 2, 'o'), ('O', 'c', 2, 3),
    ('g', 1, 2, 'o'), ('O', 't', 3, 2), ('u', 2), ('g', 2, 2, 'o'), ('A', 5), ('F', 't', 4, 0, 1),
    ('F', 't', 4, 1, 0), ('g', 0, 2, 'f'), ('O', 't', 2, 3), ('P', 't', 4, 0, 1), ('P', 't', 4, 1, 0), ('F', 't', 4, 2, 1),
    ('g', 1, 2, 'f'), ('g', 2, 2, 'f'), ('P', 't', 4, 2, 1), ('B', 5), ('F', 'c', 5, 0, 0), ('F', 'c', 5, 1, 1),
    ('O', 'c', 3, 3), ('P', 'c', 5, 0, 0), ('P', 'c', 5, 1, 1), ('F', 'c', 5, 2, 0), ('g', 0, 1, 'o'), ('P', 'c', 5, 2, 0),
    ('O', 'c', 2, 4), ('g', 1, 1, 'o'), ('g', 2, 1, 'o'), ('O', 't', 3, 3), ('u', 3), ('g', 3, 2, 'o'),
    ('F', 't', 5, 0, 1), ('F', 't', 5, 1, 0), ('g', 0, 1, 'f'), ('O', 't', 2, 4), ('P', 't', 5, 0, 1), ('P', 't', 5, 1, 0),
    ('F', 't', 5, 2, 1), ('P', 't', 5, 2, 1), ('g', 1, 1, 'f'), ('g', 2, 1, 'f'), ('g', 3, 2, 'f'), ('O', 'c', 3, 4),
    ('O', 'c', 2, 5), ('g', 0, 0, 'o'), ('O', 't', 3, 4), ('u', 4), ('g', 4, 2, 'o'), ('g', 3, 1, 'o'),
    ('O', 't', 2, 5), ('g', 1, 0, 'o'), ('g', 4, 2, 'f'), ('O', 'c', 3, 5), ('g', 3, 1, 'f'), ('g', 0, 0, 'f'),
    ('O', 't', 3, 5), ('u', 5), ('g', 5, 2, 'o'), ('g', 4, 1, 'o'), ('g', 1, 0, 'f'), ('g', 5, 2, 'f'),
    ('g', 4, 1, 'f'), ('g', 2, 0, 'o'), ('g', 5, 1, 'o'), ('g', 3, 0, 'o'), ('g', 5, 1, 'f'), ('g', 2, 0, 'f'),
    ('g', 3, 0, 'f'), ('g', 4, 0, 'o'), ('g', 5, 0, 'o'), ('g', 4, 0, 'f'), ('g', 5, 0, 'f'),
)


def backward_kernel(names, by_down1, h0, h1, by_y, a_t, gate1, up1, act0, gate0, up0, *refs):
    refs = list(refs)
    pop = lambda n: [refs.pop(0) for _ in range(n)]
    weights, blocks, moments, whole, new = pop(3), pop(3), [pop(2) for _ in range(3)], pop(6), [pop(2) for _ in range(3)]
    by_gate1, by_up1, by_gate0, by_up0, by_down0, hid_gate, hid_up = pop(7)
    away = pop(18)
    states, turned, start_sem = pop(3)
    sems = pop(5)
    has = dict(zip(names, away + refs, strict=True))
    w_gate, w_up, w_down = weights
    it = Sums([by_down1, by_gate1, by_up1, by_down0, by_gate0, by_up0], has)
    (tokens, d), hidden = h0.shape, gate0.shape[1]
    tall, wide = pl.BlockSpec((WIDTH, d), lambda i: (i, 0)), pl.BlockSpec((d, WIDTH), lambda i: (0, i))
    across = pl.BlockSpec((tokens, WIDTH), lambda i: (0, i))
    cut = pl.BlockSpec((4, 4, 4, 3, 8, WIDTH), lambda i: (0, 0, 0, 0, 0, i))
    packed = pl.BlockSpec((1, 2, 4, *WIDE), lambda i: (i // 2, lax.rem(i, 2), 0, 0, 0, 0))

    def do(op):
        if op[0] in "AB":
            it.send(*op)
        elif op[0] == "F":
            it.fetch(*op[1:])
        elif op[0] == "P":
            it.first(*op[1:])
        else:
            it.later(*op[1:])

    def loop(stage, body, ins, outs, *at):
        def hook(sub):
            for (tile, where), ops in PLAN[stage].items():
                if where == sub:
                    @pl.when(pl.program_id(0) == tile)
                    def _():
                        for op in ops:
                            do(op)

        pltpu.emit_pipeline(functools.partial(body, hook), grid=(hidden // WIDTH,), in_specs=ins, out_specs=outs)(*at)

    def into(hook, gate, up, w_down, by_gate_w, hid_up, *hid_gate):
        hook(0)
        g, u = gate[...], up[...]
        by_act = dot(states[...], w_down[...], (1, 1)).astype(BF).astype(F32)
        part = jax.nn.sigmoid(g)
        silu = g * part
        hid_up[...] = (by_act * silu).astype(BF)
        by_gate = (by_act * u * (part + silu * (1 - part))).astype(BF)
        if hid_gate:
            hid_gate[0][...] = by_gate
        by_gate_w[...] = dot(turned[...], by_gate).reshape(by_gate_w.shape).astype(BF)
        hook(1)

    def of_up(hook, by_up, by_up_w):
        hook(0)
        by_up_w[...] = dot(turned[...], by_up[...]).reshape(by_up_w.shape).astype(BF)

    def down(hook, act, by_w):
        hook(0)
        pack(by_w, dot(act[...], states[...], (0, 0)))

    def back_to_states(acc, late0, late1, late_sem):
        acc[...] = jnp.zeros_like(acc)

        def more(hook, by_gate, by_up, w_gate, w_up):
            hook(0)
            acc[...] += dot(by_gate[...], w_gate[...], (1, 1)) + dot(by_up[...], w_up[...], (1, 1))

        loop("mid", more, [across, across, wide, wide], [], hid_gate, hid_up, w_gate.at[1], w_up.at[1])
        def copies(r):
            rows, slot = pl.ds(pl.multiple_of(128 * r, 128), 128), lax.rem(r, 2)
            return [pltpu.make_async_copy(ref.at[rows], buf.at[slot], late_sem.at[slot, i]) for i, (ref, buf) in enumerate(((h0, late0), (h1, late1)))]

        for copy in copies(0):
            copy.start()

        @over(tokens // 128)
        def _(r):
            for (tile, _), ops in PLAN["turn"].items():
                @pl.when(r == 2 * tile)
                def _():
                    for op in ops:
                        do(op)

            @pl.when(r + 1 < tokens // 128)
            def _():
                for copy in copies(r + 1):
                    copy.start()

            for copy in copies(r):
                copy.wait()
            rows, slot = pl.ds(pl.multiple_of(128 * r, 128), 128), lax.rem(r, 2)
            turned[:, rows] = normed(late0[slot]).T
            states[rows] = normed_back(late1[slot], acc[rows].astype(BF), states[rows])

    def tail(*bufs):
        last = Gather(it, blocks, moments, whole, new, dict(zip(gather_scratch(), bufs, strict=True)), sems)
        for m in range(len(ORDER)):
            for copy in last.loads(m):
                copy.start()
        for op in TAIL:
            if op[0] == "u":
                last.adamw(op[1])
            elif op[0] == "g":
                last.send(op[1], op[2], op[3] == "f")
            else:
                do(op)
        it.end(0, 5)
        last.end()

    early = [pltpu.make_async_copy(by_y, states, start_sem.at[0]), pltpu.make_async_copy(a_t, turned, start_sem.at[1])]
    for copy in early:
        copy.start()
    greet(it.left, it.right)
    for op in PLAN["start"][0, 0]:
        do(op)
    for copy in early:
        copy.wait()
    loop("top", into, [across, across, tall], [cut, across, across], gate1, up1, w_down.at[1], by_gate1, hid_up, hid_gate)
    loop("up", of_up, [across], [cut], hid_up, by_up1)
    pl.run_scoped(back_to_states, pltpu.VMEM((tokens, d), F32), *[pltpu.VMEM((2, 128, d), BF)] * 2, pltpu.SemaphoreType.DMA((2, 2)))
    loop("down", down, [across], [packed], act0, by_down0)
    loop("low", into, [across, across, tall], [cut, across], gate0, up0, w_down.at[0], by_gate0, hid_up)
    loop("last", of_up, [across], [cut], hid_up, by_up0)
    pl.run_scoped(tail, *gather_scratch().values())


def backward(by_down1, states, hidden_states, weights, moments, cid):
    near, away = sums_scratch(6)
    tokens, d = states[0].shape
    hidden = weights[0].shape[2]
    args = [by_down1.reshape(4, 4, 4, *WIDE), *states, *hidden_states, *weights, *(w.reshape(2, 64, *BLOCK[k]) for w, k in zip(weights, KINDS)), *(t.reshape(2, *BLOCK[k]) for pair, k in zip(moments, KINDS) for t in pair)]
    across = jax.ShapeDtypeStruct((tokens, hidden), BF)
    outs = [*(jax.ShapeDtypeStruct((4, 4, 4, *BLOCK[k]), BF) for k in KIND_OF), *(jax.ShapeDtypeStruct((2, *BLOCK[k]), F32) for k in KINDS for _ in range(2)),
        *[jax.ShapeDtypeStruct((4, 4, 4, *WIDE), BF)] * 5, across, across, *away.values()]
    dma = pltpu.SemaphoreType.DMA
    scratch = [pltpu.VMEM((tokens, d), BF), pltpu.VMEM((d, tokens), BF), dma((2,)),
        dma((6, 3)), dma((6, 2)), dma((6,)), dma((6, 6)), dma((6, 6))]
    out = pl.pallas_call(
        functools.partial(backward_kernel, (*away, *near)),
        in_specs=[ANYWHERE] * len(args), out_specs=[ANYWHERE] * len(outs), out_shape=outs, scratch_shapes=scratch + list(near.values()),
        compiler_params=pltpu.CompilerParams(collective_id=cid, has_side_effects=True, vmem_limit_bytes=VMEM),
        name="backward",
    )(*args)
    return out[:6], [[t.reshape(pair[0].shape) for t in out[6 + 2 * i:8 + 2 * i]] for i, pair in enumerate(moments)]


def solution(mesh):
    def step(x, dy, *arrays):
        weights, m, v = (arrays[i : i + 3] for i in (0, 3, 6))
        layers = weights[0].shape[0]
        assert layers == 2
        h0, by_y = x[0], dy[0]
        gate0, up0, act0, h1 = forward(h0, None, weights, 0)
        gate1, up1, by_down1, a_t = forward(h1, by_y, weights, 1)
        whole, new = backward(by_down1, [h0, h1, by_y, a_t], [gate1, up1, act0, gate0, up0], weights, list(zip(m, v)), 1)
        out = [jnp.stack([whole[ORDER.index((number, i))].reshape(weights[i].shape[1:]) for number in range(layers)]) for i in range(3)]
        return (*out, *(new[i][which] for which in (0, 1) for i in range(3)))

    blocks = P(None, "dp", None)
    return jax.shard_map(step, mesh=mesh, in_specs=(P(("rep", "dp")),) * 2 + (P(),) * 3 + (blocks,) * 6,
        out_specs=(P("rep"),) * 3 + (P("rep", "dp", None),) * 6, check_vma=False)
```

```python
import functools
import jax, jax.numpy as jnp
from jax import lax
from jax.experimental import pallas as pl
from jax.experimental.pallas import tpu as pltpu
MESH = pl.DeviceIdType.MESH
BF, F32 = jnp.bfloat16, jnp.float32
ORDERS = ((0, 1, 2), (1, 2, 0), (2, 0, 1))
STRIDE = (16, 4, 1)

from jax.sharding import PartitionSpec as P

NAMES = ("w_gate", "w_up", "w_down")
KINDS = ("wide", "wide", "tall")


def place():
    me = lax.axis_index("dp")
    at = (me // 16, (me // 4) % 4, me % 4)
    def step(axis, by):
        return me + (lax.rem(at[axis] + by, 4) - at[axis]) * STRIDE[axis]
    right = [step(a, 1) for a in range(3)]
    left = [step(a, 3) for a in range(3)]
    return at, left, right

def greet(left, right):
    barrier = pltpu.get_barrier_semaphore()
    for to in (*left, *right):
        pl.semaphore_signal(barrier, inc=1, device_id={"dp": to}, device_id_type=MESH)
    pl.semaphore_wait(barrier, 6)

def piece(kind, color, half):
    if kind == "wide":
        return (color, slice(None), slice(None) if half is None else pl.ds(2048 * half, 2048))
    return (slice(None), slice(None), pl.ds(512 * color, 512) if half is None else pl.ds(512 * color + 256 * half, 256))

BLOCK = {"wide": (3, 8, 4096), "tall": (8, 8, 1536)}
PIECE = (8, 2048)


def over(n):
    def run(body):
        lax.fori_loop(0, n, lambda i, _: body(i), None)

    return run


WIDE = BLOCK["wide"]
VMEM = 67043328


def sums_scratch(n):
    near, away = {}, {}
    for m in range(n):
        for phase, lead in ((1, (3, 2, 4, 4)), (2, (3, 2, 4)), (3, (3, 2))):
            for letter in "ABC":
                if phase == 1:
                    away[f"{letter}1", m] = jax.ShapeDtypeStruct((*lead, *PIECE), BF)
                else:
                    near[f"{letter}{phase}", m] = pltpu.VMEM((*lead, *PIECE), BF)
    near["pass1"] = pltpu.VMEM((3, 2, 4, 4, *PIECE), BF)
    for phase, lead in ((2, (3, 2, 4)), (3, (3, 2))):
        near[f"send{phase}"] = pltpu.VMEM((2, *lead, *PIECE), BF)
        near[f"keep{phase}"] = pltpu.VMEM((2, *lead, *PIECE), F32)
    near["G"] = pltpu.VMEM((n, 3, 2, *PIECE), BF)
    near["land"] = pltpu.VMEM((2, 3, 2, 4, 4, *PIECE), BF)
    dma = pltpu.SemaphoreType.DMA
    near |= {"land_sem": dma((2,)), "sent": dma((n, 9)), "came1": dma((n, 3, 3)), "came": dma((n, 6))}
    return near, away


class Sums:
    def __init__(self, src, has):
        self.src, self.has = src, has
        self.at, self.left, self.right = place()
        self.by = [[lax.rem(a + o, 4) for a in self.at] for o in range(4)]

    def own(self, m, c, o, half):
        idx = [slice(None)] * 3
        idx[ORDERS[c][0]] = self.by[o][ORDERS[c][0]]
        return self.src[m].at[(*idx, *piece("wide", c, half))]

    def copy(self, letter, phase, m, c, d):
        k = "ABC".index(letter)
        to = self.has[f"{letter}{phase}", m]
        if c is None:
            src = dst = to
        elif d is None:
            src = dst = to.at[c]
        else:
            dst = to.at[c, d]
            if letter == "C":
                src = self.has["pass1"].at[c, d] if phase == 1 else self.has[f"A{phase}", m].at[c, d]
            elif phase > 1:
                src = self.has[f"send{phase}"].at[k, c, d]
            else:
                src = self.own(m, c, *((2, d) if letter == "A" else (1 + 2 * d, 1 - d)))
        came = self.has["came1"].at[m, k, c or 0] if phase == 1 else self.has["came"].at[m, phase * 3 - 6 + k]
        return pltpu.make_async_remote_copy(src_ref=src, dst_ref=dst, send_sem=self.has["sent"].at[m, phase * 3 - 3 + k], recv_sem=came,
            device_id={"dp": (self.left if d else self.right)[ORDERS[c or 0][phase - 1]]}, device_id_type=MESH)

    def send(self, letter, m, phase=1, colors=(0, 1, 2)):
        for c in colors:
            for d in (0, 1):
                self.copy(letter, phase, m, c, d).start()

    def came(self, letters, phase, m):
        for letter in letters:
            self.copy(letter, phase, m, None, None).wait_recv()

    def sent(self, letters, phase, m):
        for letter in letters:
            self.copy(letter, phase, m, None, None).wait_send()

    def fetch(self, what, m, c, slot):
        land, sem = self.has["land"].at[slot], self.has["land_sem"].at[slot]
        for i, letter in ((0, "A"),) if what == "c" else ((0, "C"), (2, "B")):
            self.copy(letter, 1, m, c, None).wait_recv()
            pltpu.make_async_copy(self.has[f"{letter}1", m].at[c], land.at[i], sem).start()
        for d in (0, 1):
            pltpu.make_async_copy(self.own(m, c, 1 + 2 * d if what == "c" else 0, d), land.at[1, d], sem).start()

    def first(self, what, m, c, slot):
        land = self.has["land"].at[slot]
        got = land.at[0:2] if what == "c" else land
        pltpu.make_async_copy(got, got, self.has["land_sem"].at[slot]).wait()
        if what == "c":
            if m > 0 and c == 0:
                self.sent("C", 1, m - 1)
            to = self.has["pass1"]

            @over(2)
            def _(d):
                @over(4)
                def _(i):
                    @over(4)
                    def _(j):
                        to[c, d, i, j] = (land[0, d, i, j].astype(F32) + land[1, d, i, j].astype(F32)).astype(BF)

            self.send("C", m, 1, (c,))
            return
        if m > 0 and c == 0:
            self.sent("AB", 2, m - 1)
        axis = ORDERS[c][1]

        def whole(h, t, i):
            at = (t, i) if axis < ORDERS[c][2] else (i, t)
            return land[(1, h, *at)].astype(F32) + land[(0, h, *at)].astype(F32) + land[(2, 1 - h, *at)].astype(F32)

        @over(2)
        def _(h):
            @over(2)
            def _(k):
                d, t, u = self.role(axis, h, k)

                @over(4)
                def _(i):
                    self.has["send2"][k, c, d, i] = whole(h, t, i).astype(BF)
                    self.has["keep2"][k, c, h, i] = whole(h, u, i)

        self.send("A", m, 2, (c,))
        self.send("B", m, 2, (c,))

    def role(self, axis, h, k):
        turn = k * (1 - 2 * h)
        return h + turn, lax.rem(self.at[axis] + 2 + turn, 4), lax.rem(self.at[axis] + k * (1 + 2 * h), 4)

    def later(self, what, phase, m):
        a, b, c_ = (self.has[f"{letter}{phase}", m] for letter in "ABC")
        keep = self.has[f"keep{phase}"]
        if what == "c":
            self.came("A", phase, m)

            @over(3)
            def _(c):
                @over(2)
                def _(d):
                    if phase == 3:
                        a[c, d] = (a[c, d].astype(F32) + keep[1, c, d]).astype(BF)
                    else:
                        @over(4)
                        def _(i):
                            a[c, d, i] = (a[c, d, i].astype(F32) + keep[1, c, d, i]).astype(BF)

            self.send("C", m, phase)
            return
        self.came("CB", phase, m)
        if phase == 3:
            @over(3)
            def _(c):
                @over(2)
                def _(h):
                    self.has["G"][m, c, h] = (keep[0, c, h] + c_[c, h].astype(F32) + b[c, 1 - h].astype(F32)).astype(BF)

            return
        if m > 0:
            self.sent("AB", 3, m - 1)
        for c in range(3):
            def whole(h, t):
                return keep[0, c, h, t] + c_[c, h, t].astype(F32) + b[c, 1 - h, t].astype(F32)

            @over(2)
            def _(h):
                @over(2)
                def _(k):
                    d, t, u = self.role(ORDERS[c][2], h, k)
                    self.has["send3"][k, c, d] = whole(h, t).astype(BF)
                    self.has["keep3"][k, c, h] = whole(h, u)

        self.send("A", m, 3)
        self.send("B", m, 3)

    def end(self, first, last):
        for m in range(first, last + 1):
            self.sent("AB" + "C" * (m == last), 1, m)
            for phase in (2, 3):
                self.sent("C" + "AB" * (m == last), phase, m)


ORDER = ((1, 2), (1, 0), (1, 1), (0, 2), (0, 0), (0, 1))
KIND_OF = tuple(KINDS[i] for _, i in ORDER)
SLOT_OF = tuple(KIND_OF[:m].count(k) for m, k in enumerate(KIND_OF))


def gather_scratch():
    out = {}
    for kind in dict.fromkeys(KIND_OF):
        n = KIND_OF.count(kind)
        out["moments", kind] = pltpu.VMEM((n, 2, *BLOCK[kind]), F32)
        out["w", kind] = pltpu.VMEM((n, *BLOCK[kind]), BF)
    return out


class Gather:
    def __init__(self, it, weights, moments, whole, new, has, sems):
        self.it, self.weights, self.moments, self.whole, self.new, self.has = it, weights, moments, whole, new, has
        self.load_sem, self.save_sem, self.mine_sem, self.ssem, self.rsem = sems

    def held(self, m):
        return self.has["w", KIND_OF[m]].at[SLOT_OF[m]]

    def loads(self, m):
        layer, i = ORDER[m]
        me = lax.axis_index("dp")
        refs = [self.weights[i].at[layer, me], *(ref.at[layer] for ref in self.moments[i])]
        bufs = [self.held(m), *(self.has["moments", KIND_OF[m]].at[SLOT_OF[m], j] for j in (0, 1))]
        return [pltpu.make_async_copy(ref, buf, self.load_sem.at[m, j]) for j, (ref, buf) in enumerate(zip(refs, bufs))]

    def saves(self, m):
        layer, i = ORDER[m]
        return [pltpu.make_async_copy(self.has["moments", KIND_OF[m]].at[SLOT_OF[m], j], self.new[i][j].at[layer], self.save_sem.at[m, j])
            for j in (0, 1)]

    def mine(self, m):
        at = self.it.at
        return pltpu.make_async_copy(self.held(m), self.whole[m].at[at[0], at[1], at[2]], self.mine_sem.at[m])

    def adamw(self, m):
        for copy in self.loads(m):
            copy.wait()
        w, moments, g = self.held(m), self.has["moments", KIND_OF[m]].at[SLOT_OF[m]], self.it.has["G"].at[m]

        @over(3)
        def _(c):
            @over(2)
            def _(h):
                @over(4)
                def _(i):
                    from_g = (c, h, slice(None), pl.ds(pl.multiple_of(512 * i, 512), 512))
                    if KIND_OF[m] == "wide":
                        at = (c, slice(None), pl.ds(pl.multiple_of(2048 * h + 512 * i, 512), 512))
                    else:
                        at = (4 * h + i, slice(None), pl.ds(pl.multiple_of(512 * c, 512), 512))
                    w[at], moments[(0, *at)], moments[(1, *at)] = adamw(w[at].astype(F32), moments[(0, *at)], moments[(1, *at)], g[from_g].astype(F32))

        self.mine(m).start()
        for copy in self.saves(m):
            copy.start()

    def msg(self, m, color, phase, d, fwd):
        order, at = ORDERS[color], self.it.at
        axis = order[phase]
        idx = list(at)
        if fwd:
            idx[axis] = self.it.by[3 if d == 0 else 1][axis]
        for p in range(phase + 1, 3):
            idx[order[p]] = slice(None)
        part = piece(KIND_OF[m], color, d if fwd else None)
        dst = self.whole[m].at[(*idx, *part)]
        src = self.held(m).at[part] if phase == 2 and not fwd else dst
        return self.sets(m, phase, fwd, src, dst, (self.it.right if d == 0 else self.it.left)[axis])

    def sets(self, m, phase, fwd, src, dst, to):
        k = phase * 2 + int(fwd)
        return pltpu.make_async_remote_copy(src_ref=src, dst_ref=dst, send_sem=self.ssem.at[m, k], recv_sem=self.rsem.at[m, k],
            device_id={"dp": to}, device_id_type=MESH)

    def all(self, m, phase, fwd):
        much = self.whole[m].at[(*(0,) * phase, slice(0, 1 if fwd else 2))]
        return self.sets(m, phase, fwd, much, much, self.it.right[0])

    def send(self, m, phase, fwd):
        if fwd:
            self.all(m, phase, False).wait_recv()
        elif phase < 2:
            self.all(m, phase + 1, True).wait_recv()
        if not fwd and phase == 1:
            self.mine(m).wait()
        for color in range(3):
            for d in (0, 1):
                self.msg(m, color, phase, d, fwd).start()

    def end(self):
        for m in range(len(ORDER)):
            for copy in self.saves(m):
                copy.wait()
            last = int(m == len(ORDER) - 1)
            self.all(m, last, True).wait_recv()
            for phase in range(last, 3):
                for fwd in (False, True):
                    self.all(m, phase, fwd).wait_send()


def dot(a, b, over=(1, 0)):
    return lax.dot_general(a, b, ((over[:1], over[1:]), ((), ())), preferred_element_type=F32)


WIDTH = 512
ROWS = 128
ONCE = pl.Buffered(1)
ANYWHERE = pl.BlockSpec(memory_space=pl.ANY)


def normed(h):
    wide = h.astype(F32)
    scale = lax.rsqrt(jnp.mean(wide**2, -1, keepdims=True) + 1e-6)
    return (wide * scale).astype(BF)


def normed_back(h, by_a, by_h):
    wide, by_a = h.astype(F32), by_a.astype(F32)
    scale = lax.rsqrt(jnp.mean(wide**2, -1, keepdims=True) + 1e-6)
    along = jnp.mean(by_a * wide, -1, keepdims=True)
    return (by_h.astype(F32) + (by_a * scale - wide * (along * scale**3)).astype(BF).astype(F32)).astype(BF)


PACKED = pl.BlockSpec((WIDTH // 64, *WIDE), lambda i: (i, 0, 0, 0))


def specs(tokens, d, layer):
    return (pl.BlockSpec((1, WIDTH, d), lambda i: (layer, i, 0)), pl.BlockSpec((1, d, WIDTH), lambda i: (layer, 0, i)),
        pl.BlockSpec((tokens, WIDTH), lambda i: (0, i)), pl.BlockSpec((tokens, d), lambda i: (0, 0), pipeline_mode=ONCE))


def pack(out, tile):
    tile = tile.reshape(*out.shape[:-3], 8, 8, 1536)
    for c in range(3):
        for g in range(8):
            out[..., c, :, 512 * g:512 * g + 512] = tile[..., g, :, 512 * c:512 * c + 512].astype(BF)


def rows_of(ref):
    return [pl.ds(ROWS * r, ROWS) for r in range(ref.shape[0] // ROWS)]


def first_kernel(h, w_gate, w_up, w_down, gate, up, act, out, a, acc):
    tile = pl.program_id(0)

    @pl.when(tile == 0)
    def _():
        acc[...] = jnp.zeros_like(acc)
        for r in rows_of(h):
            a[r] = normed(h[r])

    g, u = dot(a[...], w_gate[0]), dot(a[...], w_up[0])
    gate[...], up[...] = g, u
    act[...] = (jax.nn.silu(g) * u).astype(BF)
    acc[...] += dot(act[...], w_down[0])

    @pl.when(tile == pl.num_programs(0) - 1)
    def _():
        for r in rows_of(h):
            out[r] = (h[r].astype(F32) + acc[r].astype(BF).astype(F32)).astype(BF)


def last_kernel(h, by_y, w_gate, w_up, gate, up, by_down, a_t, a):
    @pl.when(pl.program_id(0) == 0)
    def _():
        for r in rows_of(h):
            a[r] = normed(h[r])
            a_t[:, r] = a[r].T

    g, u = dot(a[...], w_gate[0]), dot(a[...], w_up[0])
    gate[...], up[...] = g, u
    pack(by_down, dot((jax.nn.silu(g) * u).astype(BF), by_y[...], (0, 0)))


def forward(h, by_y, weights, layer):
    (tokens, d), hidden = h.shape, weights[0].shape[2]
    w_down, w_in, across, states = specs(tokens, d, layer)
    flat, wide = jax.ShapeDtypeStruct((tokens, d), BF), jax.ShapeDtypeStruct((tokens, hidden), F32)
    call = functools.partial(pl.pallas_call, grid=(hidden // WIDTH,), compiler_params=pltpu.CompilerParams(vmem_limit_bytes=VMEM))
    if by_y is None:
        return call(first_kernel, in_specs=[states, w_in, w_in, w_down], out_specs=[across, across, across, states], out_shape=[wide, wide, jax.ShapeDtypeStruct(wide.shape, BF), flat],
            scratch_shapes=[pltpu.VMEM((tokens, d), BF), pltpu.VMEM((tokens, d), F32)], name="first")(h, *weights)
    turned = pl.BlockSpec((d, tokens), lambda i: (0, 0), pipeline_mode=ONCE)
    return call(last_kernel, in_specs=[states, states, w_in, w_in], out_specs=[across, across, PACKED, turned],
        out_shape=[wide, wide, jax.ShapeDtypeStruct((64, *WIDE), BF), jax.ShapeDtypeStruct((d, tokens), BF)],
        scratch_shapes=[pltpu.VMEM((tokens, d), BF)], name="last")(h, by_y, *weights[:2])


def adamw(w, m, v, g):
    m = 0.9 * m + 0.1 * g
    v = 0.95 * v + 0.05 * g * g
    step = m * lax.rsqrt(v + 1e-8) + 0.1 * w
    return (w - 0.02 * step).astype(BF), m, v


PLAN = {
    "start": {
        (0, 0): (('A', 0),),
    },
    "top": {
        (1, 0): (('B', 0),),
        (3, 1): (('F', 'c', 0, 0, 0), ('F', 'c', 0, 1, 1),),
        (4, 0): (('P', 'c', 0, 0, 0), ('F', 'c', 0, 2, 0),),
        (4, 1): (('P', 'c', 0, 1, 1),),
        (5, 0): (('P', 'c', 0, 2, 0),),
    },
    "up": {
        (0, 0): (('F', 't', 0, 0, 1), ('F', 't', 0, 1, 0), ('A', 1),),
        (1, 0): (('P', 't', 0, 0, 1), ('F', 't', 0, 2, 1), ('B', 1),),
        (2, 0): (('P', 't', 0, 1, 0),),
        (3, 0): (('P', 't', 0, 2, 1),),
        (6, 0): (('F', 'c', 1, 0, 0), ('F', 'c', 1, 1, 1),),
        (7, 0): (('P', 'c', 1, 0, 0), ('F', 'c', 1, 2, 0),),
    },
    "mid": {
        (0, 0): (('P', 'c', 1, 1, 1), ('A', 2),),
        (1, 0): (('P', 'c', 1, 2, 0), ('O', 'c', 2, 0),),
        (5, 0): (('F', 't', 1, 0, 1), ('F', 't', 1, 1, 0), ('B', 2),),
    },
    "turn": {
        (0, 0): (('O', 't', 2, 0),),
        (1, 0): (('P', 't', 1, 0, 1), ('F', 't', 1, 2, 1),),
        (2, 0): (('P', 't', 1, 1, 0), ('F', 'c', 2, 0, 0),),
        (3, 0): (('P', 't', 1, 2, 1), ('F', 'c', 2, 1, 1),),
    },
    "down": {
        (0, 0): (('O', 'c', 3, 0), ('P', 'c', 2, 0, 0), ('F', 'c', 2, 2, 0),),
        (1, 0): (('O', 'c', 2, 1), ('P', 'c', 2, 1, 1),),
        (2, 0): (('O', 't', 3, 0), ('P', 'c', 2, 2, 0),),
        (6, 0): (('F', 't', 2, 0, 1),),
    },
    "low": {
        (0, 0): (('O', 't', 2, 1), ('F', 't', 2, 1, 0), ('A', 3),),
        (0, 1): (('P', 't', 2, 0, 1), ('F', 't', 2, 2, 1), ('B', 3),),
        (1, 0): (('O', 'c', 3, 1), ('P', 't', 2, 1, 0),),
        (1, 1): (('P', 't', 2, 2, 1),),
        (3, 0): (('F', 'c', 3, 0, 0), ('F', 'c', 3, 1, 1),),
        (3, 1): (('P', 'c', 3, 0, 0), ('F', 'c', 3, 2, 0),),
        (4, 0): (('P', 'c', 3, 1, 1),),
        (4, 1): (('P', 'c', 3, 2, 0),),
        (5, 1): (('O', 'c', 2, 2),),
        (6, 1): (('O', 't', 3, 1),),
    },
    "last": {
        (0, 0): (('F', 't', 3, 0, 1), ('F', 't', 3, 1, 0), ('A', 4),),
        (1, 0): (('O', 't', 2, 2),),
        (2, 0): (('P', 't', 3, 0, 1), ('F', 't', 3, 2, 1), ('B', 4),),
        (3, 0): (('P', 't', 3, 1, 0),),
        (4, 0): (('P', 't', 3, 2, 1),),
        (6, 0): (('O', 'c', 3, 2), ('F', 'c', 4, 0, 0), ('F', 'c', 4, 1, 1),),
        (7, 0): (('P', 'c', 4, 0, 0), ('F', 'c', 4, 2, 0),),
    },
}
TAIL = (
    ('P', 'c', 4, 1, 1), ('P', 'c', 4, 2, 0), ('u', 0), ('u', 1), ('g', 0, 2, 'o'), ('O', 'c', 2, 3),
    ('g', 1, 2, 'o'), ('O', 't', 3, 2), ('u', 2), ('g', 2, 2, 'o'), ('A', 5), ('F', 't', 4, 0, 1),
    ('F', 't', 4, 1, 0), ('g', 0, 2, 'f'), ('O', 't', 2, 3), ('P', 't', 4, 0, 1), ('P', 't', 4, 1, 0), ('F', 't', 4, 2, 1),
    ('g', 1, 2, 'f'), ('g', 2, 2, 'f'), ('P', 't', 4, 2, 1), ('B', 5), ('F', 'c', 5, 0, 0), ('F', 'c', 5, 1, 1),
    ('O', 'c', 3, 3), ('P', 'c', 5, 0, 0), ('P', 'c', 5, 1, 1), ('F', 'c', 5, 2, 0), ('g', 0, 1, 'o'), ('P', 'c', 5, 2, 0),
    ('O', 'c', 2, 4), ('g', 1, 1, 'o'), ('g', 2, 1, 'o'), ('O', 't', 3, 3), ('u', 3), ('g', 3, 2, 'o'),
    ('F', 't', 5, 0, 1), ('F', 't', 5, 1, 0), ('g', 0, 1, 'f'), ('O', 't', 2, 4), ('P', 't', 5, 0, 1), ('P', 't', 5, 1, 0),
    ('F', 't', 5, 2, 1), ('P', 't', 5, 2, 1), ('g', 1, 1, 'f'), ('g', 2, 1, 'f'), ('g', 3, 2, 'f'), ('O', 'c', 3, 4),
    ('O', 'c', 2, 5), ('g', 0, 0, 'o'), ('O', 't', 3, 4), ('u', 4), ('g', 4, 2, 'o'), ('g', 3, 1, 'o'),
    ('O', 't', 2, 5), ('g', 1, 0, 'o'), ('g', 4, 2, 'f'), ('O', 'c', 3, 5), ('g', 3, 1, 'f'), ('g', 0, 0, 'f'),
    ('O', 't', 3, 5), ('u', 5), ('g', 5, 2, 'o'), ('g', 4, 1, 'o'), ('g', 1, 0, 'f'), ('g', 5, 2, 'f'),
    ('g', 4, 1, 'f'), ('g', 2, 0, 'o'), ('g', 5, 1, 'o'), ('g', 3, 0, 'o'), ('g', 5, 1, 'f'), ('g', 2, 0, 'f'),
    ('g', 3, 0, 'f'), ('g', 4, 0, 'o'), ('g', 4, 0, 'f'),
)


def backward_kernel(names, by_down1, h0, h1, by_y, a_t, gate1, up1, act0, gate0, up0, *refs):
    refs = list(refs)
    pop = lambda n: [refs.pop(0) for _ in range(n)]
    weights, blocks, moments, whole, new = pop(3), pop(3), [pop(2) for _ in range(3)], pop(6), [pop(2) for _ in range(3)]
    by_gate1, by_up1, by_gate0, by_up0, by_down0, hid_gate, hid_up = pop(7)
    away = pop(18)
    states, turned, start_sem = pop(3)
    sems = pop(5)
    has = dict(zip(names, away + refs, strict=True))
    w_gate, w_up, w_down = weights
    it = Sums([by_down1, by_gate1, by_up1, by_down0, by_gate0, by_up0], has)
    (tokens, d), hidden = h0.shape, gate0.shape[1]
    tall, wide = pl.BlockSpec((WIDTH, d), lambda i: (i, 0)), pl.BlockSpec((d, WIDTH), lambda i: (0, i))
    across = pl.BlockSpec((tokens, WIDTH), lambda i: (0, i))
    cut = pl.BlockSpec((4, 4, 4, 3, 8, WIDTH), lambda i: (0, 0, 0, 0, 0, i))
    packed = pl.BlockSpec((1, 2, 4, *WIDE), lambda i: (i // 2, lax.rem(i, 2), 0, 0, 0, 0))

    def do(op):
        if op[0] in "AB":
            it.send(*op)
        elif op[0] == "F":
            it.fetch(*op[1:])
        elif op[0] == "P":
            it.first(*op[1:])
        else:
            it.later(*op[1:])

    def loop(stage, body, ins, outs, *at):
        def hook(sub):
            for (tile, where), ops in PLAN[stage].items():
                if where == sub:
                    @pl.when(pl.program_id(0) == tile)
                    def _():
                        for op in ops:
                            do(op)

        pltpu.emit_pipeline(functools.partial(body, hook), grid=(hidden // WIDTH,), in_specs=ins, out_specs=outs)(*at)

    def into(hook, gate, up, w_down, by_gate_w, hid_up, by_gate):
        hook(0)
        for r in [pl.ds(256 * i, 256) for i in range(tokens // 256)]:
            g, u = gate[r], up[r]
            by_act = dot(states[r], w_down[...], (1, 1)).astype(BF).astype(F32)
            part = jax.nn.sigmoid(g)
            silu = g * part
            hid_up[r] = (by_act * silu).astype(BF)
            by_gate[r] = (by_act * u * (part + silu * (1 - part))).astype(BF)
        by_gate_w[...] = dot(turned[...], by_gate[...]).reshape(by_gate_w.shape).astype(BF)
        hook(1)

    def of_up(hook, by_up, by_up_w):
        hook(0)
        by_up_w[...] = dot(turned[...], by_up[...]).reshape(by_up_w.shape).astype(BF)

    def down(hook, act, by_w):
        hook(0)
        pack(by_w, dot(act[...], states[...], (0, 0)))

    def back_to_states(acc, late0, late1, late_sem):
        acc[...] = jnp.zeros_like(acc)

        def more(hook, by_gate, by_up, w_gate, w_up):
            hook(0)
            acc[...] += dot(by_gate[...], w_gate[...], (1, 1)) + dot(by_up[...], w_up[...], (1, 1))

        loop("mid", more, [across, across, wide, wide], [], hid_gate, hid_up, w_gate.at[1], w_up.at[1])
        def copies(r):
            rows, slot = pl.ds(pl.multiple_of(128 * r, 128), 128), lax.rem(r, 2)
            return [pltpu.make_async_copy(ref.at[rows], buf.at[slot], late_sem.at[slot, i]) for i, (ref, buf) in enumerate(((h0, late0), (h1, late1)))]

        for copy in copies(0):
            copy.start()

        @over(tokens // 128)
        def _(r):
            for (tile, _), ops in PLAN["turn"].items():
                @pl.when(r == 2 * tile)
                def _():
                    for op in ops:
                        do(op)

            @pl.when(r + 1 < tokens // 128)
            def _():
                for copy in copies(r + 1):
                    copy.start()

            for copy in copies(r):
                copy.wait()
            rows, slot = pl.ds(pl.multiple_of(128 * r, 128), 128), lax.rem(r, 2)
            turned[:, rows] = normed(late0[slot]).T
            states[rows] = normed_back(late1[slot], acc[rows].astype(BF), states[rows])

    def tail(*bufs):
        last = Gather(it, blocks, moments, whole, new, dict(zip(gather_scratch(), bufs, strict=True)), sems)
        for m in range(len(ORDER)):
            for copy in last.loads(m):
                copy.start()
        for op in TAIL:
            if op[0] == "u":
                last.adamw(op[1])
            elif op[0] == "g":
                last.send(op[1], op[2], op[3] == "f")
            else:
                do(op)
        it.end(0, 5)
        last.end()

    early = [pltpu.make_async_copy(by_y, states, start_sem.at[0]), pltpu.make_async_copy(a_t, turned, start_sem.at[1])]
    for copy in early:
        copy.start()
    greet(it.left, it.right)
    for op in PLAN["start"][0, 0]:
        do(op)
    for copy in early:
        copy.wait()
    loop("top", into, [across, across, tall], [cut, across, across], gate1, up1, w_down.at[1], by_gate1, hid_up, hid_gate)
    loop("up", of_up, [across], [cut], hid_up, by_up1)
    pl.run_scoped(back_to_states, pltpu.VMEM((tokens, d), F32), *[pltpu.VMEM((2, 128, d), BF)] * 2, pltpu.SemaphoreType.DMA((2, 2)))
    loop("down", down, [across], [packed], act0, by_down0)
    loop("low", into, [across, across, tall], [cut, across, across], gate0, up0, w_down.at[0], by_gate0, hid_up, hid_gate)
    loop("last", of_up, [across], [cut], hid_up, by_up0)
    pl.run_scoped(tail, *gather_scratch().values())


def backward(by_down1, states, hidden_states, weights, moments, cid):
    near, away = sums_scratch(6)
    tokens, d = states[0].shape
    hidden = weights[0].shape[2]
    args = [by_down1.reshape(4, 4, 4, *WIDE), *states, *hidden_states, *weights, *(w.reshape(2, 64, *BLOCK[k]) for w, k in zip(weights, KINDS)), *(t.reshape(2, *BLOCK[k]) for pair, k in zip(moments, KINDS) for t in pair)]
    across = jax.ShapeDtypeStruct((tokens, hidden), BF)
    outs = [*(jax.ShapeDtypeStruct((4, 4, 4, *BLOCK[k]), BF) for k in KIND_OF), *(jax.ShapeDtypeStruct((2, *BLOCK[k]), F32) for k in KINDS for _ in range(2)),
        *[jax.ShapeDtypeStruct((4, 4, 4, *WIDE), BF)] * 5, across, across, *away.values()]
    dma = pltpu.SemaphoreType.DMA
    scratch = [pltpu.VMEM((tokens, d), BF), pltpu.VMEM((d, tokens), BF), dma((2,)),
        dma((6, 3)), dma((6, 2)), dma((6,)), dma((6, 6)), dma((6, 6))]
    out = pl.pallas_call(
        functools.partial(backward_kernel, (*away, *near)),
        in_specs=[ANYWHERE] * len(args), out_specs=[ANYWHERE] * len(outs), out_shape=outs, scratch_shapes=scratch + list(near.values()),
        compiler_params=pltpu.CompilerParams(collective_id=cid, has_side_effects=True, vmem_limit_bytes=VMEM),
        name="backward",
    )(*args)
    return out[:6], [out[6 + 2 * i:8 + 2 * i] for i in range(3)]


AHEAD = 6


class Move:
    def __init__(self, sems):
        self.in_sem, self.out_sem = sems
        self.moves, self.used = [], {}

    def add(self, source, ring, slots, place):
        self.used[id(ring)] = slot = (self.used.get(id(ring), -1) + 1) % slots
        self.moves.append((source, ring.at[slot] if slots > 1 else ring, place, (id(ring), slot)))

    def copies(self, i):
        source, slot, place, _ = self.moves[i]
        return pltpu.make_async_copy(source, slot, self.in_sem.at[i]), pltpu.make_async_copy(slot, place, self.out_sem.at[i])

    def run(self):
        n, stored = len(self.moves), set()
        for i in range(n + AHEAD):
            if i < n:
                for j in range(i):
                    if j not in stored and self.moves[j][3] == self.moves[i][3]:
                        self.copies(j)[1].wait()
                        stored.add(j)
                self.copies(i)[0].start()
            if 0 <= i - AHEAD < n:
                into, out = self.copies(i - AHEAD)
                into.wait()
                out.start()
        for i in range(n):
            if i not in stored:
                self.copies(i)[1].wait()


def settle_kernel(*refs):
    whole, new, outs, news, rings, held, sems = refs[:4], refs[4:10], refs[10:12], refs[12:18], refs[18:20], refs[20:26], refs[26:]
    move = Move(sems)
    for m, array in zip(EARLY, whole):
        layer, i = ORDER[m]
        for x in range(4):
            for y in (0, 2):
                move.add(array.at[x, pl.ds(y, 2)], rings[i // 2], 2 * AHEAD, outs[i // 2].at[layer, x, pl.ds(y, 2)])
    for source, buf, place in zip(new, held, news):
        move.add(source, buf, 1, place)
    move.run()


def settle_last_kernel(*refs):
    one, own, came, out, rings, sems = refs[0], refs[1], refs[2:11], refs[11], refs[12:14], refs[14:]
    at, move = place()[0], Move(sems)
    for x in range(4):
        for y in (0, 2):
            move.add(one.at[x, pl.ds(y, 2)], rings[0], 2 * AHEAD, out.at[1, x, pl.ds(y, 2)])
    for c in range(3):
        axis = ORDERS[c][0]
        for k in range(4):
            idx = [slice(None)] * 3
            idx[axis] = lax.rem(at[axis] + 4 - k, 4)
            move.add(own.at[(*idx, c)] if k == 0 else came[3 * c + k - 1], rings[1], 2 * AHEAD, out.at[(0, *idx, c)])
    move.run()


EARLY = (1, 4, 0, 3)


def settle(whole, new):
    me, last = lax.axis_index("dp"), whole[5]
    at = (me // 16, (me // 4) % 4, me % 4)
    came = []
    for c in range(3):
        axis = ORDERS[c][0]
        start, size = [0, 0, 0, c, 0, 0], [4, 4, 4, 1, 8, 4096]
        start[axis], size[axis] = at[axis], 1
        mine = lax.dynamic_slice(last, start, size).reshape(4, 4, 8, 4096)
        for k in (1, 2, 3):
            ring = [(i, i + ((i // STRIDE[axis] + k) % 4 - i // STRIDE[axis] % 4) * STRIDE[axis]) for i in range(64)]
            came.append(lax.ppermute(mine, "dp", ring))
    flat = [t for pair in new for t in pair]
    dma = pltpu.SemaphoreType.DMA
    both = {k: jax.ShapeDtypeStruct((2, 4, 4, 4, *BLOCK[k]), BF) for k in ("wide", "tall")}
    ring = {k: pltpu.VMEM((2 * AHEAD, 2, 4, *BLOCK[k]), BF) for k in ("wide", "tall")}
    call = functools.partial(pl.pallas_call, compiler_params=pltpu.CompilerParams(vmem_limit_bytes=VMEM),
        cost_estimate=pl.CostEstimate(flops=60000000000, bytes_accessed=110000000, transcendentals=0))
    gate, down, *flat = call(settle_kernel, in_specs=[ANYWHERE] * 10, out_specs=[ANYWHERE] * 8,
        out_shape=[both["wide"], both["tall"], *(jax.ShapeDtypeStruct(t.shape, t.dtype) for t in flat)],
        scratch_shapes=[ring["wide"], ring["tall"], *(pltpu.VMEM(t.shape, t.dtype) for t in flat), dma((38,)), dma((38,))], name="settle",
    )(*(whole[m] for m in EARLY), *flat)
    up = call(settle_last_kernel, in_specs=[ANYWHERE] * 11, out_specs=ANYWHERE, out_shape=both["wide"],
        scratch_shapes=[ring["wide"], pltpu.VMEM((2 * AHEAD, 4, 4, 8, 4096), BF), dma((20,)), dma((20,))], name="settle_last",
    )(whole[2], last, *came)
    return [gate, up, down], [flat[2 * i:2 * i + 2] for i in range(3)]


def solution(mesh):
    def step(x, dy, *arrays):
        weights, m, v = (arrays[i : i + 3] for i in (0, 3, 6))
        layers = weights[0].shape[0]
        assert layers == 2
        h0, by_y = x[0], dy[0]
        gate0, up0, act0, h1 = forward(h0, None, weights, 0)
        gate1, up1, by_down1, a_t = forward(h1, by_y, weights, 1)
        whole, new = backward(by_down1, [h0, h1, by_y, a_t], [gate1, up1, act0, gate0, up0], weights, list(zip(m, v)), 1)
        out, new = settle(whole, new)
        out = [t.reshape(w.shape) for t, w in zip(out, weights)]
        new = [[t.reshape(a.shape) for t in pair] for pair, a in zip(new, m)]
        return (*out, *(new[i][which] for which in (0, 1) for i in range(3)))

    blocks = P(None, "dp", None)
    return jax.shard_map(step, mesh=mesh, in_specs=(P(("rep", "dp")),) * 2 + (P(),) * 3 + (blocks,) * 6,
        out_specs=(P("rep"),) * 3 + (P("rep", "dp", None),) * 6, check_vma=False)
```

```python
import functools
import jax, jax.numpy as jnp
from jax import lax
from jax.experimental import pallas as pl
from jax.experimental.pallas import tpu as pltpu
MESH = pl.DeviceIdType.MESH
BF, F32 = jnp.bfloat16, jnp.float32
ORDERS = ((0, 1, 2), (1, 2, 0), (2, 0, 1))
STRIDE = (16, 4, 1)

from jax.sharding import PartitionSpec as P

NAMES = ("w_gate", "w_up", "w_down")
KINDS = ("wide", "wide", "tall")


def place():
    me = lax.axis_index("dp")
    at = (me // 16, (me // 4) % 4, me % 4)
    def step(axis, by):
        return me + (lax.rem(at[axis] + by, 4) - at[axis]) * STRIDE[axis]
    right = [step(a, 1) for a in range(3)]
    left = [step(a, 3) for a in range(3)]
    return at, left, right

def greet(left, right):
    barrier = pltpu.get_barrier_semaphore()
    for to in (*left, *right):
        pl.semaphore_signal(barrier, inc=1, device_id={"dp": to}, device_id_type=MESH)
    pl.semaphore_wait(barrier, 6)

def piece(kind, color, half):
    if kind == "wide":
        return (color, slice(None), slice(None) if half is None else pl.ds(2048 * half, 2048))
    return (slice(None), slice(None), pl.ds(512 * color, 512) if half is None else pl.ds(512 * color + 256 * half, 256))

BLOCK = {"wide": (3, 8, 4096), "tall": (8, 8, 1536)}
PIECE = (8, 2048)


def over(n):
    def run(body):
        lax.fori_loop(0, n, lambda i, _: body(i), None)

    return run


WIDE = BLOCK["wide"]
VMEM = 67043328


def sums_scratch(n):
    near, away = {}, {}
    for m in range(n):
        for phase, lead in ((1, (3, 2, 4, 4)), (2, (3, 2, 4)), (3, (3, 2))):
            for letter in "ABC":
                if phase == 1:
                    away[f"{letter}1", m] = jax.ShapeDtypeStruct((*lead, *PIECE), BF)
                else:
                    near[f"{letter}{phase}", m] = pltpu.VMEM((*lead, *PIECE), BF)
    near["pass1"] = pltpu.VMEM((3, 2, 4, 4, *PIECE), BF)
    for phase, lead in ((2, (3, 2, 4)), (3, (3, 2))):
        near[f"send{phase}"] = pltpu.VMEM((2, *lead, *PIECE), BF)
        near[f"keep{phase}"] = pltpu.VMEM((2, *lead, *PIECE), F32)
    near["G"] = pltpu.VMEM((n, 3, 2, *PIECE), BF)
    near["land"] = pltpu.VMEM((2, 3, 2, 4, 4, *PIECE), BF)
    dma = pltpu.SemaphoreType.DMA
    near |= {"land_sem": dma((2,)), "sent": dma((n, 9)), "came1": dma((n, 3, 3)), "came": dma((n, 6))}
    return near, away


class Sums:
    def __init__(self, src, has):
        self.src, self.has = src, has
        self.at, self.left, self.right = place()
        self.by = [[lax.rem(a + o, 4) for a in self.at] for o in range(4)]

    def own(self, m, c, o, half):
        idx = [slice(None)] * 3
        idx[ORDERS[c][0]] = self.by[o][ORDERS[c][0]]
        return self.src[m].at[(*idx, *piece("wide", c, half))]

    def copy(self, letter, phase, m, c, d):
        k = "ABC".index(letter)
        to = self.has[f"{letter}{phase}", m]
        if c is None:
            src = dst = to
        elif d is None:
            src = dst = to.at[c]
        else:
            dst = to.at[c, d]
            if letter == "C":
                src = self.has["pass1"].at[c, d] if phase == 1 else self.has[f"A{phase}", m].at[c, d]
            elif phase > 1:
                src = self.has[f"send{phase}"].at[k, c, d]
            else:
                src = self.own(m, c, *((2, d) if letter == "A" else (1 + 2 * d, 1 - d)))
        came = self.has["came1"].at[m, k, c or 0] if phase == 1 else self.has["came"].at[m, phase * 3 - 6 + k]
        return pltpu.make_async_remote_copy(src_ref=src, dst_ref=dst, send_sem=self.has["sent"].at[m, phase * 3 - 3 + k], recv_sem=came,
            device_id={"dp": (self.left if d else self.right)[ORDERS[c or 0][phase - 1]]}, device_id_type=MESH)

    def send(self, letter, m, phase=1, colors=(0, 1, 2)):
        for c in colors:
            for d in (0, 1):
                self.copy(letter, phase, m, c, d).start()

    def came(self, letters, phase, m):
        for letter in letters:
            self.copy(letter, phase, m, None, None).wait_recv()

    def sent(self, letters, phase, m):
        for letter in letters:
            self.copy(letter, phase, m, None, None).wait_send()

    def fetch(self, what, m, c, slot):
        land, sem = self.has["land"].at[slot], self.has["land_sem"].at[slot]
        for i, letter in ((0, "A"),) if what == "c" else ((0, "C"), (2, "B")):
            self.copy(letter, 1, m, c, None).wait_recv()
            pltpu.make_async_copy(self.has[f"{letter}1", m].at[c], land.at[i], sem).start()
        for d in (0, 1):
            pltpu.make_async_copy(self.own(m, c, 1 + 2 * d if what == "c" else 0, d), land.at[1, d], sem).start()

    def first(self, what, m, c, slot):
        land = self.has["land"].at[slot]
        got = land.at[0:2] if what == "c" else land
        pltpu.make_async_copy(got, got, self.has["land_sem"].at[slot]).wait()
        if what == "c":
            if m > 0 and c == 0:
                self.sent("C", 1, m - 1)
            to = self.has["pass1"]

            @over(2)
            def _(d):
                @over(4)
                def _(i):
                    @over(4)
                    def _(j):
                        to[c, d, i, j] = (land[0, d, i, j].astype(F32) + land[1, d, i, j].astype(F32)).astype(BF)

            self.send("C", m, 1, (c,))
            return
        if m > 0 and c == 0:
            self.sent("AB", 2, m - 1)
        axis = ORDERS[c][1]

        def whole(h, t, i):
            at = (t, i) if axis < ORDERS[c][2] else (i, t)
            return land[(1, h, *at)].astype(F32) + land[(0, h, *at)].astype(F32) + land[(2, 1 - h, *at)].astype(F32)

        @over(2)
        def _(h):
            @over(2)
            def _(k):
                d, t, u = self.role(axis, h, k)

                @over(4)
                def _(i):
                    self.has["send2"][k, c, d, i] = whole(h, t, i).astype(BF)
                    self.has["keep2"][k, c, h, i] = whole(h, u, i)

        self.send("A", m, 2, (c,))
        self.send("B", m, 2, (c,))

    def role(self, axis, h, k):
        turn = k * (1 - 2 * h)
        return h + turn, lax.rem(self.at[axis] + 2 + turn, 4), lax.rem(self.at[axis] + k * (1 + 2 * h), 4)

    def later(self, what, phase, m):
        a, b, c_ = (self.has[f"{letter}{phase}", m] for letter in "ABC")
        keep = self.has[f"keep{phase}"]
        if what == "c":
            self.came("A", phase, m)

            @over(3)
            def _(c):
                @over(2)
                def _(d):
                    if phase == 3:
                        a[c, d] = (a[c, d].astype(F32) + keep[1, c, d]).astype(BF)
                    else:
                        @over(4)
                        def _(i):
                            a[c, d, i] = (a[c, d, i].astype(F32) + keep[1, c, d, i]).astype(BF)

            self.send("C", m, phase)
            return
        self.came("CB", phase, m)
        if phase == 3:
            @over(3)
            def _(c):
                @over(2)
                def _(h):
                    self.has["G"][m, c, h] = (keep[0, c, h] + c_[c, h].astype(F32) + b[c, 1 - h].astype(F32)).astype(BF)

            return
        if m > 0:
            self.sent("AB", 3, m - 1)
        for c in range(3):
            def whole(h, t):
                return keep[0, c, h, t] + c_[c, h, t].astype(F32) + b[c, 1 - h, t].astype(F32)

            @over(2)
            def _(h):
                @over(2)
                def _(k):
                    d, t, u = self.role(ORDERS[c][2], h, k)
                    self.has["send3"][k, c, d] = whole(h, t).astype(BF)
                    self.has["keep3"][k, c, h] = whole(h, u)

        self.send("A", m, 3)
        self.send("B", m, 3)

    def end(self, first, last):
        for m in range(first, last + 1):
            self.sent("AB" + "C" * (m == last), 1, m)
            for phase in (2, 3):
                self.sent("C" + "AB" * (m == last), phase, m)


ORDER = ((1, 2), (1, 0), (1, 1), (0, 2), (0, 0), (0, 1))
KIND_OF = tuple(KINDS[i] for _, i in ORDER)
SLOT_OF = tuple(KIND_OF[:m].count(k) for m, k in enumerate(KIND_OF))


def gather_scratch():
    out = {}
    for kind in dict.fromkeys(KIND_OF):
        n = KIND_OF.count(kind)
        out["moments", kind] = pltpu.VMEM((n, 2, *BLOCK[kind]), F32)
        out["w", kind] = pltpu.VMEM((n, *BLOCK[kind]), BF)
    return out


class Gather:
    def __init__(self, it, weights, moments, whole, new, has, sems):
        self.it, self.weights, self.moments, self.whole, self.new, self.has = it, weights, moments, whole, new, has
        self.load_sem, self.save_sem, self.mine_sem, self.ssem, self.rsem = sems

    def held(self, m):
        return self.has["w", KIND_OF[m]].at[SLOT_OF[m]]

    def loads(self, m):
        layer, i = ORDER[m]
        me = lax.axis_index("dp")
        refs = [self.weights[i].at[layer, me], *(ref.at[layer] for ref in self.moments[i])]
        bufs = [self.held(m), *(self.has["moments", KIND_OF[m]].at[SLOT_OF[m], j] for j in (0, 1))]
        return [pltpu.make_async_copy(ref, buf, self.load_sem.at[m, j]) for j, (ref, buf) in enumerate(zip(refs, bufs))]

    def saves(self, m):
        layer, i = ORDER[m]
        return [pltpu.make_async_copy(self.has["moments", KIND_OF[m]].at[SLOT_OF[m], j], self.new[i][j].at[layer], self.save_sem.at[m, j])
            for j in (0, 1)]

    def mine(self, m):
        at = self.it.at
        return pltpu.make_async_copy(self.held(m), self.whole[m].at[at[0], at[1], at[2]], self.mine_sem.at[m])

    def adamw(self, m):
        for copy in self.loads(m):
            copy.wait()
        w, moments, g = self.held(m), self.has["moments", KIND_OF[m]].at[SLOT_OF[m]], self.it.has["G"].at[m]

        @over(3)
        def _(c):
            @over(2)
            def _(h):
                @over(4)
                def _(i):
                    from_g = (c, h, slice(None), pl.ds(pl.multiple_of(512 * i, 512), 512))
                    if KIND_OF[m] == "wide":
                        at = (c, slice(None), pl.ds(pl.multiple_of(2048 * h + 512 * i, 512), 512))
                    else:
                        at = (4 * h + i, slice(None), pl.ds(pl.multiple_of(512 * c, 512), 512))
                    w[at], moments[(0, *at)], moments[(1, *at)] = adamw(w[at].astype(F32), moments[(0, *at)], moments[(1, *at)], g[from_g].astype(F32))

        self.mine(m).start()
        for copy in self.saves(m):
            copy.start()

    def msg(self, m, color, phase, d, fwd):
        order, at = ORDERS[color], self.it.at
        axis = order[phase]
        idx = list(at)
        if fwd:
            idx[axis] = self.it.by[3 if d == 0 else 1][axis]
        for p in range(phase + 1, 3):
            idx[order[p]] = slice(None)
        part = piece(KIND_OF[m], color, d if fwd else None)
        dst = self.whole[m].at[(*idx, *part)]
        src = self.held(m).at[part] if phase == 2 and not fwd else dst
        return self.sets(m, phase, fwd, src, dst, (self.it.right if d == 0 else self.it.left)[axis])

    def sets(self, m, phase, fwd, src, dst, to):
        k = phase * 2 + int(fwd)
        return pltpu.make_async_remote_copy(src_ref=src, dst_ref=dst, send_sem=self.ssem.at[m, k], recv_sem=self.rsem.at[m, k],
            device_id={"dp": to}, device_id_type=MESH)

    def own_set(self, color):
        axis = ORDERS[color][0]
        idx = [slice(None)] * 3
        idx[axis] = self.it.at[axis]
        return self.whole[-1].at[(*idx, color)]

    def all(self, m, phase, fwd):
        much = self.whole[m].at[(*(0,) * phase, slice(0, 1 if fwd else 2))]
        return self.sets(m, phase, fwd, much, much, self.it.right[0])

    def send(self, m, phase, fwd):
        if fwd:
            self.all(m, phase, False).wait_recv()
        elif phase < 2:
            self.all(m, phase + 1, True).wait_recv()
        if not fwd and phase == 1:
            self.mine(m).wait()
        for color in range(3):
            for d in (0, 1):
                self.msg(m, color, phase, d, fwd).start()

    def end(self):
        for m in range(len(ORDER)):
            for copy in self.saves(m):
                copy.wait()
            last = int(m == len(ORDER) - 1)
            if not last:
                self.all(m, 0, True).wait_recv()
            for phase in range(last, 3):
                for fwd in (False, True):
                    self.all(m, phase, fwd).wait_send()


def dot(a, b, over=(1, 0)):
    return lax.dot_general(a, b, ((over[:1], over[1:]), ((), ())), preferred_element_type=F32)


WIDTH = 512
ROWS = 128
ONCE = pl.Buffered(1)
ANYWHERE = pl.BlockSpec(memory_space=pl.ANY)


def normed(h):
    wide = h.astype(F32)
    scale = lax.rsqrt(jnp.mean(wide**2, -1, keepdims=True) + 1e-6)
    return (wide * scale).astype(BF)


def normed_back(h, by_a, by_h):
    wide, by_a = h.astype(F32), by_a.astype(F32)
    scale = lax.rsqrt(jnp.mean(wide**2, -1, keepdims=True) + 1e-6)
    along = jnp.mean(by_a * wide, -1, keepdims=True)
    return (by_h.astype(F32) + (by_a * scale - wide * (along * scale**3)).astype(BF).astype(F32)).astype(BF)


PACKED = pl.BlockSpec((WIDTH // 64, *WIDE), lambda i: (i, 0, 0, 0))


def specs(tokens, d, layer):
    return (pl.BlockSpec((1, WIDTH, d), lambda i: (layer, i, 0)), pl.BlockSpec((1, d, WIDTH), lambda i: (layer, 0, i)),
        pl.BlockSpec((tokens, WIDTH), lambda i: (0, i)), pl.BlockSpec((tokens, d), lambda i: (0, 0), pipeline_mode=ONCE))


def pack(out, tile):
    tile = tile.reshape(*out.shape[:-3], 8, 8, 1536)
    for c in range(3):
        for g in range(8):
            out[..., c, :, 512 * g:512 * g + 512] = tile[..., g, :, 512 * c:512 * c + 512].astype(BF)


def rows_of(ref):
    return [pl.ds(ROWS * r, ROWS) for r in range(ref.shape[0] // ROWS)]


def first_kernel(h, w_gate, w_up, w_down, gate, up, act, out, a, acc):
    tile = pl.program_id(0)

    @pl.when(tile == 0)
    def _():
        acc[...] = jnp.zeros_like(acc)
        for r in rows_of(h):
            a[r] = normed(h[r])

    g, u = dot(a[...], w_gate[0]), dot(a[...], w_up[0])
    gate[...], up[...] = g, u
    act[...] = (jax.nn.silu(g) * u).astype(BF)
    acc[...] += dot(act[...], w_down[0])

    @pl.when(tile == pl.num_programs(0) - 1)
    def _():
        for r in rows_of(h):
            out[r] = (h[r].astype(F32) + acc[r].astype(BF).astype(F32)).astype(BF)


def last_kernel(h, by_y, w_gate, w_up, gate, up, by_down, a_t, a):
    @pl.when(pl.program_id(0) == 0)
    def _():
        for r in rows_of(h):
            a[r] = normed(h[r])
            a_t[:, r] = a[r].T

    g, u = dot(a[...], w_gate[0]), dot(a[...], w_up[0])
    gate[...], up[...] = g, u
    pack(by_down, dot((jax.nn.silu(g) * u).astype(BF), by_y[...], (0, 0)))


def forward(h, by_y, weights, layer):
    (tokens, d), hidden = h.shape, weights[0].shape[2]
    w_down, w_in, across, states = specs(tokens, d, layer)
    flat, wide = jax.ShapeDtypeStruct((tokens, d), BF), jax.ShapeDtypeStruct((tokens, hidden), F32)
    call = functools.partial(pl.pallas_call, grid=(hidden // WIDTH,), compiler_params=pltpu.CompilerParams(vmem_limit_bytes=VMEM))
    if by_y is None:
        return call(first_kernel, in_specs=[states, w_in, w_in, w_down], out_specs=[across, across, across, states], out_shape=[wide, wide, jax.ShapeDtypeStruct(wide.shape, BF), flat],
            scratch_shapes=[pltpu.VMEM((tokens, d), BF), pltpu.VMEM((tokens, d), F32)], name="first")(h, *weights)
    turned = pl.BlockSpec((d, tokens), lambda i: (0, 0), pipeline_mode=ONCE)
    return call(last_kernel, in_specs=[states, states, w_in, w_in], out_specs=[across, across, PACKED, turned],
        out_shape=[wide, wide, jax.ShapeDtypeStruct((64, *WIDE), BF), jax.ShapeDtypeStruct((d, tokens), BF)],
        scratch_shapes=[pltpu.VMEM((tokens, d), BF)], name="last")(h, by_y, *weights[:2])


def adamw(w, m, v, g):
    m = 0.9 * m + 0.1 * g
    v = 0.95 * v + 0.05 * g * g
    step = m * lax.rsqrt(v + 1e-8) + 0.1 * w
    return (w - 0.02 * step).astype(BF), m, v


PLAN = {
    "start": {
        (0, 0): (('A', 0),),
    },
    "top": {
        (1, 0): (('B', 0),),
        (4, 1): (('F', 'c', 0, 0, 0), ('F', 'c', 0, 1, 1),),
        (5, 0): (('P', 'c', 0, 0, 0), ('F', 'c', 0, 2, 0),),
        (5, 1): (('P', 'c', 0, 1, 1),),
        (6, 0): (('P', 'c', 0, 2, 0),),
    },
    "up": {
        (0, 0): (('A', 1),),
        (1, 0): (('F', 't', 0, 0, 1),),
        (2, 0): (('P', 't', 0, 0, 1), ('F', 't', 0, 1, 0), ('B', 1),),
        (3, 0): (('P', 't', 0, 1, 0), ('F', 't', 0, 2, 1),),
        (4, 0): (('P', 't', 0, 2, 1),),
        (7, 0): (('F', 'c', 1, 0, 0), ('F', 'c', 1, 1, 1),),
    },
    "mid": {
        (0, 0): (('P', 'c', 1, 0, 0), ('F', 'c', 1, 2, 0), ('A', 2),),
        (1, 0): (('P', 'c', 1, 1, 1),),
        (2, 0): (('P', 'c', 1, 2, 0), ('O', 'c', 2, 0),),
        (6, 0): (('F', 't', 1, 0, 1), ('B', 2),),
    },
    "turn": {
        (2, 0): (('F', 't', 1, 1, 0),),
        (3, 0): (('O', 't', 2, 0),),
    },
    "down": {
        (0, 0): (('P', 't', 1, 0, 1), ('F', 't', 1, 2, 1),),
        (1, 0): (('P', 't', 1, 1, 0), ('F', 'c', 2, 0, 0),),
        (2, 0): (('P', 't', 1, 2, 1), ('O', 'c', 3, 0),),
        (3, 0): (('P', 'c', 2, 0, 0), ('F', 'c', 2, 1, 1), ('F', 'c', 2, 2, 0),),
        (4, 0): (('P', 'c', 2, 1, 1),),
        (5, 0): (('O', 'c', 2, 1), ('P', 'c', 2, 2, 0),),
        (7, 0): (('O', 't', 3, 0),),
    },
    "low": {
        (0, 0): (('A', 3),),
        (1, 1): (('F', 't', 2, 0, 1), ('F', 't', 2, 1, 0), ('B', 3),),
        (2, 0): (('O', 't', 2, 1),),
        (2, 1): (('P', 't', 2, 0, 1), ('F', 't', 2, 2, 1),),
        (3, 0): (('P', 't', 2, 1, 0),),
        (3, 1): (('P', 't', 2, 2, 1), ('F', 'c', 3, 0, 0), ('F', 'c', 3, 1, 1),),
        (4, 0): (('P', 'c', 3, 0, 0), ('F', 'c', 3, 2, 0),),
        (4, 1): (('P', 'c', 3, 1, 1),),
        (5, 0): (('P', 'c', 3, 2, 0),),
        (6, 1): (('O', 'c', 3, 1),),
        (7, 1): (('O', 'c', 2, 2),),
    },
    "last": {
        (0, 0): (('A', 4),),
        (3, 0): (('F', 't', 3, 0, 1), ('F', 't', 3, 1, 0),),
        (4, 0): (('O', 't', 3, 1), ('B', 4),),
        (6, 0): (('O', 't', 2, 2),),
        (7, 0): (('P', 't', 3, 0, 1), ('F', 't', 3, 2, 1),),
    },
}
TAIL = (
    ('P', 't', 3, 1, 0), ('P', 't', 3, 2, 1), ('F', 'c', 4, 0, 0), ('F', 'c', 4, 1, 1), ('P', 'c', 4, 0, 0), ('P', 'c', 4, 1, 1),
    ('F', 'c', 4, 2, 0), ('u', 0), ('P', 'c', 4, 2, 0), ('u', 1), ('g', 0, 2, 'o'), ('g', 1, 2, 'o'),
    ('O', 'c', 3, 2), ('O', 'c', 2, 3), ('A', 5), ('F', 't', 4, 0, 1), ('F', 't', 4, 1, 0), ('B', 5),
    ('g', 0, 2, 'f'), ('O', 't', 3, 2), ('u', 2), ('g', 1, 2, 'f'), ('g', 2, 2, 'o'), ('O', 't', 2, 3),
    ('P', 't', 4, 0, 1), ('P', 't', 4, 1, 0), ('F', 't', 4, 2, 1), ('P', 't', 4, 2, 1), ('F', 'c', 5, 0, 0), ('F', 'c', 5, 1, 1),
    ('P', 'c', 5, 0, 0), ('P', 'c', 5, 1, 1), ('F', 'c', 5, 2, 0), ('P', 'c', 5, 2, 0), ('g', 0, 1, 'o'), ('g', 1, 1, 'o'),
    ('O', 'c', 3, 3), ('g', 2, 2, 'f'), ('O', 'c', 2, 4), ('F', 't', 5, 0, 1), ('F', 't', 5, 1, 0), ('g', 0, 1, 'f'),
    ('O', 't', 3, 3), ('u', 3), ('g', 3, 2, 'o'), ('g', 1, 1, 'f'), ('g', 2, 1, 'o'), ('O', 't', 2, 4),
    ('P', 't', 5, 0, 1), ('P', 't', 5, 1, 0), ('F', 't', 5, 2, 1), ('P', 't', 5, 2, 1), ('g', 3, 2, 'f'), ('g', 0, 0, 'o'),
    ('O', 'c', 3, 4), ('g', 2, 1, 'f'), ('O', 'c', 2, 5), ('g', 3, 1, 'o'), ('O', 't', 3, 4), ('u', 4),
    ('g', 4, 2, 'o'), ('g', 0, 0, 'f'), ('O', 't', 2, 5), ('g', 3, 1, 'f'), ('g', 4, 2, 'f'), ('g', 1, 0, 'o'),
    ('O', 'c', 3, 5), ('g', 4, 1, 'o'), ('g', 2, 0, 'o'), ('O', 't', 3, 5), ('u', 5), ('g', 5, 2, 'o'),
    ('g', 4, 1, 'f'), ('g', 1, 0, 'f'), ('g', 5, 2, 'f'), ('g', 2, 0, 'f'), ('g', 5, 1, 'o'), ('g', 3, 0, 'o'),
    ('g', 5, 1, 'f'), ('g', 4, 0, 'o'), ('g', 3, 0, 'f'), ('g', 4, 0, 'f'),
)


def backward_kernel(names, by_down1, h0, h1, by_y, a_t, gate1, up1, act0, gate0, up0, *refs):
    refs = list(refs)
    pop = lambda n: [refs.pop(0) for _ in range(n)]
    weights, blocks, moments, whole, new = pop(3), pop(3), [pop(2) for _ in range(3)], pop(6), [pop(2) for _ in range(3)]
    sets = pop(3)
    by_gate1, by_up1, by_gate0, by_up0, by_down0, hid_gate, hid_up = pop(7)
    away = pop(18)
    states, turned, start_sem = pop(3)
    sems = pop(5)
    has = dict(zip(names, away + refs, strict=True))
    w_gate, w_up, w_down = weights
    it = Sums([by_down1, by_gate1, by_up1, by_down0, by_gate0, by_up0], has)
    (tokens, d), hidden = h0.shape, gate0.shape[1]
    tall, wide = pl.BlockSpec((WIDTH, d), lambda i: (i, 0)), pl.BlockSpec((d, WIDTH), lambda i: (0, i))
    across = pl.BlockSpec((tokens, WIDTH), lambda i: (0, i))
    cut = pl.BlockSpec((4, 4, 4, 3, 8, WIDTH), lambda i: (0, 0, 0, 0, 0, i))
    packed = pl.BlockSpec((1, 2, 4, *WIDE), lambda i: (i // 2, lax.rem(i, 2), 0, 0, 0, 0))

    def do(op):
        if op[0] in "AB":
            it.send(*op)
        elif op[0] == "F":
            it.fetch(*op[1:])
        elif op[0] == "P":
            it.first(*op[1:])
        else:
            it.later(*op[1:])

    def loop(stage, body, ins, outs, *at):
        def hook(sub):
            for (tile, where), ops in PLAN[stage].items():
                if where == sub:
                    @pl.when(pl.program_id(0) == tile)
                    def _():
                        for op in ops:
                            do(op)

        pltpu.emit_pipeline(functools.partial(body, hook), grid=(hidden // WIDTH,), in_specs=ins, out_specs=outs)(*at)

    def into(hook, gate, up, w_down, by_gate_w, hid_up, by_gate):
        hook(0)
        for r in [pl.ds(256 * i, 256) for i in range(tokens // 256)]:
            g, u = gate[r], up[r]
            by_act = dot(states[r], w_down[...], (1, 1)).astype(BF).astype(F32)
            part = jax.nn.sigmoid(g)
            silu = g * part
            hid_up[r] = (by_act * silu).astype(BF)
            by_gate[r] = (by_act * u * (part + silu * (1 - part))).astype(BF)
        by_gate_w[...] = dot(turned[...], by_gate[...]).reshape(by_gate_w.shape).astype(BF)
        hook(1)

    def of_up(hook, by_up, by_up_w):
        hook(0)
        by_up_w[...] = dot(turned[...], by_up[...]).reshape(by_up_w.shape).astype(BF)

    def down(hook, act, by_w):
        hook(0)
        pack(by_w, dot(act[...], states[...], (0, 0)))

    def back_to_states(acc, late0, late1, late_sem):
        acc[...] = jnp.zeros_like(acc)

        def more(hook, by_gate, by_up, w_gate, w_up):
            hook(0)
            acc[...] += dot(by_gate[...], w_gate[...], (1, 1)) + dot(by_up[...], w_up[...], (1, 1))

        loop("mid", more, [across, across, wide, wide], [], hid_gate, hid_up, w_gate.at[1], w_up.at[1])
        def copies(r):
            rows, slot = pl.ds(pl.multiple_of(128 * r, 128), 128), lax.rem(r, 2)
            return [pltpu.make_async_copy(ref.at[rows], buf.at[slot], late_sem.at[slot, i]) for i, (ref, buf) in enumerate(((h0, late0), (h1, late1)))]

        for copy in copies(0):
            copy.start()

        @over(tokens // 128)
        def _(r):
            for (tile, _), ops in PLAN["turn"].items():
                @pl.when(r == 2 * tile)
                def _():
                    for op in ops:
                        do(op)

            @pl.when(r + 1 < tokens // 128)
            def _():
                for copy in copies(r + 1):
                    copy.start()

            for copy in copies(r):
                copy.wait()
            rows, slot = pl.ds(pl.multiple_of(128 * r, 128), 128), lax.rem(r, 2)
            turned[:, rows] = normed(late0[slot]).T
            states[rows] = normed_back(late1[slot], acc[rows].astype(BF), states[rows])

    def tail(aside, aside_sem, *bufs):
        last = Gather(it, blocks, moments, whole, new, dict(zip(gather_scratch(), bufs, strict=True)), sems)
        for m in range(len(ORDER)):
            for copy in last.loads(m):
                copy.start()
        for op in TAIL:
            if op[0] == "u":
                last.adamw(op[1])
            elif op[0] == "g":
                last.send(op[1], op[2], op[3] == "f")
            else:
                do(op)
        last.all(5, 1, True).wait_recv()
        into = [pltpu.make_async_copy(last.own_set(c), aside.at[c], aside_sem.at[c]) for c in range(3)]
        out = [pltpu.make_async_copy(aside.at[c], sets[c], aside_sem.at[c]) for c in range(3)]
        for copy in into:
            copy.start()
        for one, two in zip(into, out):
            one.wait()
            two.start()
        it.end(0, 5)
        last.end()
        for copy in out:
            copy.wait()

    early = [pltpu.make_async_copy(by_y, states, start_sem.at[0]), pltpu.make_async_copy(a_t, turned, start_sem.at[1])]
    for copy in early:
        copy.start()
    greet(it.left, it.right)
    for op in PLAN["start"][0, 0]:
        do(op)
    for copy in early:
        copy.wait()
    loop("top", into, [across, across, tall], [cut, across, across], gate1, up1, w_down.at[1], by_gate1, hid_up, hid_gate)
    loop("up", of_up, [across], [cut], hid_up, by_up1)
    pl.run_scoped(back_to_states, pltpu.VMEM((tokens, d), F32), *[pltpu.VMEM((2, 128, d), BF)] * 2, pltpu.SemaphoreType.DMA((2, 2)))
    loop("down", down, [across], [packed], act0, by_down0)
    loop("low", into, [across, across, tall], [cut, across, across], gate0, up0, w_down.at[0], by_gate0, hid_up, hid_gate)
    loop("last", of_up, [across], [cut], hid_up, by_up0)
    pl.run_scoped(tail, pltpu.VMEM((3, 4, 4, 8, 4096), BF), pltpu.SemaphoreType.DMA((3,)), *gather_scratch().values())


def backward(by_down1, states, hidden_states, weights, moments, cid):
    near, away = sums_scratch(6)
    tokens, d = states[0].shape
    hidden = weights[0].shape[2]
    args = [by_down1.reshape(4, 4, 4, *WIDE), *states, *hidden_states, *weights, *(w.reshape(2, 64, *BLOCK[k]) for w, k in zip(weights, KINDS)), *(t.reshape(2, *BLOCK[k]) for pair, k in zip(moments, KINDS) for t in pair)]
    across = jax.ShapeDtypeStruct((tokens, hidden), BF)
    outs = [*(jax.ShapeDtypeStruct((4, 4, 4, *BLOCK[k]), BF) for k in KIND_OF), *(jax.ShapeDtypeStruct((2, *BLOCK[k]), F32) for k in KINDS for _ in range(2)), *[jax.ShapeDtypeStruct((4, 4, 8, 4096), BF)] * 3,
        *[jax.ShapeDtypeStruct((4, 4, 4, *WIDE), BF)] * 5, across, across, *away.values()]
    dma = pltpu.SemaphoreType.DMA
    scratch = [pltpu.VMEM((tokens, d), BF), pltpu.VMEM((d, tokens), BF), dma((2,)),
        dma((6, 3)), dma((6, 2)), dma((6,)), dma((6, 6)), dma((6, 6))]
    out = pl.pallas_call(
        functools.partial(backward_kernel, (*away, *near)),
        in_specs=[ANYWHERE] * len(args), out_specs=[ANYWHERE] * len(outs), out_shape=outs, scratch_shapes=scratch + list(near.values()),
        compiler_params=pltpu.CompilerParams(collective_id=cid, has_side_effects=True, vmem_limit_bytes=VMEM),
        name="backward",
    )(*args)
    return out[:5], [out[6 + 2 * i:8 + 2 * i] for i in range(3)], out[12:15]


AHEAD = 6


class Move:
    def __init__(self, sems):
        self.in_sem, self.out_sem = sems
        self.moves, self.used = [], {}

    def add(self, source, ring, slots, place):
        self.used[id(ring)] = slot = (self.used.get(id(ring), -1) + 1) % slots
        self.moves.append((source, ring.at[slot] if slots > 1 else ring, place, (id(ring), slot)))

    def copies(self, i):
        source, slot, place, _ = self.moves[i]
        return pltpu.make_async_copy(source, slot, self.in_sem.at[i]), pltpu.make_async_copy(slot, place, self.out_sem.at[i])

    def run(self):
        n, stored = len(self.moves), set()
        for i in range(n + AHEAD):
            if i < n:
                for j in range(i):
                    if j not in stored and self.moves[j][3] == self.moves[i][3]:
                        self.copies(j)[1].wait()
                        stored.add(j)
                self.copies(i)[0].start()
            if 0 <= i - AHEAD < n:
                into, out = self.copies(i - AHEAD)
                into.wait()
                out.start()
        for i in range(n):
            if i not in stored:
                self.copies(i)[1].wait()


def settle_kernel(*refs):
    whole, new, outs, news, rings, held, sems = refs[:5], refs[5:11], refs[11:14], refs[14:20], refs[20:22], refs[22:28], refs[28:]
    move = Move(sems)
    for (layer, i), array in zip(ORDER, whole):
        for x in range(4):
            for y in (0, 2):
                move.add(array.at[x, pl.ds(y, 2)], rings[i // 2], 2 * AHEAD, outs[i].at[layer, x, pl.ds(y, 2)])
    for source, buf, place in zip(new, held, news):
        move.add(source, buf, 1, place)
    move.run()


def settle_last_kernel(_, *refs):
    sets, came, out, ring, sems = refs[:3], refs[3:12], refs[12], refs[13], refs[14:]
    at, move = place()[0], Move(sems)
    for c in range(3):
        axis = ORDERS[c][0]
        for k in range(4):
            idx = [slice(None)] * 3
            idx[axis] = lax.rem(at[axis] + 4 - k, 4)
            move.add(came[3 * c + k - 1] if k else sets[c], ring, 2 * AHEAD, out.at[(0, *idx, c)])
    move.run()


def settle(whole, new, sets):
    came = []
    for c in range(3):
        stride = STRIDE[ORDERS[c][0]]
        for k in (2, 1, 3):
            ring = [(i, i + ((i // stride + k) % 4 - i // stride % 4) * stride) for i in range(64)]
            came.append((3 * c + k - 1, lax.ppermute(sets[c], "dp", ring)))
    flat = [t for pair in new for t in pair]
    dma = pltpu.SemaphoreType.DMA
    both = {k: jax.ShapeDtypeStruct((2, 4, 4, 4, *BLOCK[k]), BF) for k in ("wide", "tall")}
    ring = {k: pltpu.VMEM((2 * AHEAD, 2, 4, *BLOCK[k]), BF) for k in ("wide", "tall")}
    call = functools.partial(pl.pallas_call, compiler_params=pltpu.CompilerParams(vmem_limit_bytes=VMEM),
        cost_estimate=pl.CostEstimate(flops=60000000000, bytes_accessed=130000000, transcendentals=0))
    gate, up, down, *flat = call(settle_kernel, in_specs=[ANYWHERE] * 11, out_specs=[ANYWHERE] * 9,
        out_shape=[both["wide"], both["wide"], both["tall"], *(jax.ShapeDtypeStruct(t.shape, t.dtype) for t in flat)],
        scratch_shapes=[ring["wide"], ring["tall"], *(pltpu.VMEM(t.shape, t.dtype) for t in flat), dma((46,)), dma((46,))], name="settle",
    )(*whole, *flat)
    up = call(settle_last_kernel, in_specs=[ANYWHERE] * 13, out_specs=ANYWHERE, out_shape=both["wide"], input_output_aliases={0: 0},
        scratch_shapes=[pltpu.VMEM((2 * AHEAD, 4, 4, 8, 4096), BF), dma((12,)), dma((12,))], name="settle_last",
    )(up, *sets, *(t for _, t in sorted(came, key=lambda one: one[0])))
    return [gate, up, down], [flat[2 * i:2 * i + 2] for i in range(3)]


def solution(mesh):
    def step(x, dy, *arrays):
        weights, m, v = (arrays[i : i + 3] for i in (0, 3, 6))
        layers = weights[0].shape[0]
        assert layers == 2
        h0, by_y = x[0], dy[0]
        gate0, up0, act0, h1 = forward(h0, None, weights, 0)
        gate1, up1, by_down1, a_t = forward(h1, by_y, weights, 1)
        whole, new, sets = backward(by_down1, [h0, h1, by_y, a_t], [gate1, up1, act0, gate0, up0], weights, list(zip(m, v)), 1)
        out, new = settle(whole, new, sets)
        out = [t.reshape(w.shape) for t, w in zip(out, weights)]
        new = [[t.reshape(a.shape) for t in pair] for pair, a in zip(new, m)]
        return (*out, *(new[i][which] for which in (0, 1) for i in range(3)))

    blocks = P(None, "dp", None)
    return jax.shard_map(step, mesh=mesh, in_specs=(P(("rep", "dp")),) * 2 + (P(),) * 3 + (blocks,) * 6,
        out_specs=(P("rep"),) * 3 + (P("rep", "dp", None),) * 6, check_vma=False)
```

```python
import functools
import jax, jax.numpy as jnp
from jax import lax
from jax.experimental import pallas as pl
from jax.experimental.pallas import tpu as pltpu
MESH = pl.DeviceIdType.MESH
BF, F32 = jnp.bfloat16, jnp.float32
ORDERS = ((0, 1, 2), (1, 2, 0), (2, 0, 1))
STRIDE = (16, 4, 1)

from jax.sharding import PartitionSpec as P

NAMES = ("w_gate", "w_up", "w_down")
KINDS = ("wide", "wide", "tall")


def place():
    me = lax.axis_index("dp")
    at = (me // 16, (me // 4) % 4, me % 4)
    def step(axis, by):
        return me + (lax.rem(at[axis] + by, 4) - at[axis]) * STRIDE[axis]
    right = [step(a, 1) for a in range(3)]
    left = [step(a, 3) for a in range(3)]
    return at, left, right

def greet(left, right):
    barrier = pltpu.get_barrier_semaphore()
    for to in (*left, *right):
        pl.semaphore_signal(barrier, inc=1, device_id={"dp": to}, device_id_type=MESH)
    pl.semaphore_wait(barrier, 6)

def piece(kind, color, half):
    if kind == "wide":
        return (color, slice(None), slice(None) if half is None else pl.ds(2048 * half, 2048))
    return (slice(None), slice(None), pl.ds(512 * color, 512) if half is None else pl.ds(512 * color + 256 * half, 256))

BLOCK = {"wide": (3, 8, 4096), "tall": (8, 8, 1536)}
PIECE = (8, 2048)


def over(n):
    def run(body):
        lax.fori_loop(0, n, lambda i, _: body(i), None)

    return run


WIDE = BLOCK["wide"]
VMEM = 67043328


def sums_scratch(n):
    near, away = {}, {}
    for m in range(n):
        for phase, lead in ((1, (3, 2, 4, 4)), (2, (3, 2, 4)), (3, (3, 2))):
            for letter in "ABC":
                if phase == 1:
                    away[f"{letter}1", m] = jax.ShapeDtypeStruct((*lead, *PIECE), BF)
                else:
                    near[f"{letter}{phase}", m] = pltpu.VMEM((*lead, *PIECE), BF)
    near["pass1"] = pltpu.VMEM((3, 2, 4, 4, *PIECE), BF)
    for phase, lead in ((2, (3, 2, 4)), (3, (3, 2))):
        near[f"send{phase}"] = pltpu.VMEM((2, *lead, *PIECE), BF)
        near[f"keep{phase}"] = pltpu.VMEM((2, *lead, *PIECE), F32)
    near["G"] = pltpu.VMEM((n, 3, 2, *PIECE), BF)
    near["land"] = pltpu.VMEM((2, 3, 2, 4, 4, *PIECE), BF)
    dma = pltpu.SemaphoreType.DMA
    near |= {"land_sem": dma((2,)), "sent": dma((n, 9)), "came1": dma((n, 3, 3)), "came": dma((n, 6))}
    return near, away


class Sums:
    def __init__(self, src, has):
        self.src, self.has = src, has
        self.at, self.left, self.right = place()
        self.by = [[lax.rem(a + o, 4) for a in self.at] for o in range(4)]

    def own(self, m, c, o, half):
        idx = [slice(None)] * 3
        idx[ORDERS[c][0]] = self.by[o][ORDERS[c][0]]
        return self.src[m].at[(*idx, *piece("wide", c, half))]

    def copy(self, letter, phase, m, c, d):
        k = "ABC".index(letter)
        to = self.has[f"{letter}{phase}", m]
        if c is None:
            src = dst = to
        elif d is None:
            src = dst = to.at[c]
        else:
            dst = to.at[c, d]
            if letter == "C":
                src = self.has["pass1"].at[c, d] if phase == 1 else self.has[f"A{phase}", m].at[c, d]
            elif phase > 1:
                src = self.has[f"send{phase}"].at[k, c, d]
            else:
                src = self.own(m, c, *((2, d) if letter == "A" else (1 + 2 * d, 1 - d)))
        came = self.has["came1"].at[m, k, c or 0] if phase == 1 else self.has["came"].at[m, phase * 3 - 6 + k]
        return pltpu.make_async_remote_copy(src_ref=src, dst_ref=dst, send_sem=self.has["sent"].at[m, phase * 3 - 3 + k], recv_sem=came,
            device_id={"dp": (self.left if d else self.right)[ORDERS[c or 0][phase - 1]]}, device_id_type=MESH)

    def send(self, letter, m, phase=1, colors=(0, 1, 2)):
        for c in colors:
            for d in (0, 1):
                self.copy(letter, phase, m, c, d).start()

    def came(self, letters, phase, m):
        for letter in letters:
            self.copy(letter, phase, m, None, None).wait_recv()

    def sent(self, letters, phase, m):
        for letter in letters:
            self.copy(letter, phase, m, None, None).wait_send()

    def fetch(self, what, m, c, slot):
        land, sem = self.has["land"].at[slot], self.has["land_sem"].at[slot]
        for i, letter in ((0, "A"),) if what == "c" else ((0, "C"), (2, "B")):
            self.copy(letter, 1, m, c, None).wait_recv()
            pltpu.make_async_copy(self.has[f"{letter}1", m].at[c], land.at[i], sem).start()
        for d in (0, 1):
            pltpu.make_async_copy(self.own(m, c, 1 + 2 * d if what == "c" else 0, d), land.at[1, d], sem).start()

    def first(self, what, m, c, slot):
        land = self.has["land"].at[slot]
        got = land.at[0:2] if what == "c" else land
        pltpu.make_async_copy(got, got, self.has["land_sem"].at[slot]).wait()
        if what == "c":
            if m > 0 and c == 0:
                self.sent("C", 1, m - 1)
            to = self.has["pass1"]

            @over(2)
            def _(d):
                @over(4)
                def _(i):
                    @over(4)
                    def _(j):
                        to[c, d, i, j] = (land[0, d, i, j].astype(F32) + land[1, d, i, j].astype(F32)).astype(BF)

            self.send("C", m, 1, (c,))
            return
        if m > 0 and c == 0:
            self.sent("AB", 2, m - 1)
        axis = ORDERS[c][1]

        def whole(h, t, i):
            at = (t, i) if axis < ORDERS[c][2] else (i, t)
            return land[(1, h, *at)].astype(F32) + land[(0, h, *at)].astype(F32) + land[(2, 1 - h, *at)].astype(F32)

        @over(2)
        def _(h):
            @over(2)
            def _(k):
                d, t, u = self.role(axis, h, k)

                @over(4)
                def _(i):
                    self.has["send2"][k, c, d, i] = whole(h, t, i).astype(BF)
                    self.has["keep2"][k, c, h, i] = whole(h, u, i)

        self.send("A", m, 2, (c,))
        self.send("B", m, 2, (c,))

    def role(self, axis, h, k):
        turn = k * (1 - 2 * h)
        return h + turn, lax.rem(self.at[axis] + 2 + turn, 4), lax.rem(self.at[axis] + k * (1 + 2 * h), 4)

    def later(self, what, phase, m):
        a, b, c_ = (self.has[f"{letter}{phase}", m] for letter in "ABC")
        keep = self.has[f"keep{phase}"]
        if what == "c":
            self.came("A", phase, m)

            @over(3)
            def _(c):
                @over(2)
                def _(d):
                    if phase == 3:
                        a[c, d] = (a[c, d].astype(F32) + keep[1, c, d]).astype(BF)
                    else:
                        @over(4)
                        def _(i):
                            a[c, d, i] = (a[c, d, i].astype(F32) + keep[1, c, d, i]).astype(BF)

            self.send("C", m, phase)
            return
        self.came("CB", phase, m)
        if phase == 3:
            @over(3)
            def _(c):
                @over(2)
                def _(h):
                    self.has["G"][m, c, h] = (keep[0, c, h] + c_[c, h].astype(F32) + b[c, 1 - h].astype(F32)).astype(BF)

            return
        if m > 0:
            self.sent("AB", 3, m - 1)
        for c in range(3):
            def whole(h, t):
                return keep[0, c, h, t] + c_[c, h, t].astype(F32) + b[c, 1 - h, t].astype(F32)

            @over(2)
            def _(h):
                @over(2)
                def _(k):
                    d, t, u = self.role(ORDERS[c][2], h, k)
                    self.has["send3"][k, c, d] = whole(h, t).astype(BF)
                    self.has["keep3"][k, c, h] = whole(h, u)

        self.send("A", m, 3)
        self.send("B", m, 3)

    def end(self, first, last):
        for m in range(first, last + 1):
            self.sent("AB" + "C" * (m == last), 1, m)
            for phase in (2, 3):
                self.sent("C" + "AB" * (m == last), phase, m)


ORDER = ((1, 2), (1, 0), (1, 1), (0, 2), (0, 0), (0, 1))
KIND_OF = tuple(KINDS[i] for _, i in ORDER)
SLOT_OF = tuple(KIND_OF[:m].count(k) for m, k in enumerate(KIND_OF))


def gather_scratch():
    out = {}
    for kind in dict.fromkeys(KIND_OF):
        n = KIND_OF.count(kind)
        out["moments", kind] = pltpu.VMEM((n, 2, *BLOCK[kind]), F32)
        out["w", kind] = pltpu.VMEM((n, *BLOCK[kind]), BF)
    return out


class Gather:
    def __init__(self, it, weights, moments, whole, new, has, sems):
        self.it, self.weights, self.moments, self.whole, self.new, self.has = it, weights, moments, whole, new, has
        self.load_sem, self.save_sem, self.mine_sem, self.ssem, self.rsem = sems

    def held(self, m):
        return self.has["w", KIND_OF[m]].at[SLOT_OF[m]]

    def loads(self, m):
        layer, i = ORDER[m]
        me = lax.axis_index("dp")
        refs = [self.weights[i].at[layer, me], *(ref.at[layer] for ref in self.moments[i])]
        bufs = [self.held(m), *(self.has["moments", KIND_OF[m]].at[SLOT_OF[m], j] for j in (0, 1))]
        return [pltpu.make_async_copy(ref, buf, self.load_sem.at[m, j]) for j, (ref, buf) in enumerate(zip(refs, bufs))]

    def saves(self, m):
        layer, i = ORDER[m]
        return [pltpu.make_async_copy(self.has["moments", KIND_OF[m]].at[SLOT_OF[m], j], self.new[i][j].at[layer], self.save_sem.at[m, j])
            for j in (0, 1)]

    def mine(self, m):
        at = self.it.at
        return pltpu.make_async_copy(self.held(m), self.whole[m].at[at[0], at[1], at[2]], self.mine_sem.at[m])

    def adamw(self, m):
        for copy in self.loads(m):
            copy.wait()
        w, moments, g = self.held(m), self.has["moments", KIND_OF[m]].at[SLOT_OF[m]], self.it.has["G"].at[m]

        @over(3)
        def _(c):
            @over(2)
            def _(h):
                @over(4)
                def _(i):
                    from_g = (c, h, slice(None), pl.ds(pl.multiple_of(512 * i, 512), 512))
                    if KIND_OF[m] == "wide":
                        at = (c, slice(None), pl.ds(pl.multiple_of(2048 * h + 512 * i, 512), 512))
                    else:
                        at = (4 * h + i, slice(None), pl.ds(pl.multiple_of(512 * c, 512), 512))
                    w[at], moments[(0, *at)], moments[(1, *at)] = adamw(w[at].astype(F32), moments[(0, *at)], moments[(1, *at)], g[from_g].astype(F32))

        self.mine(m).start()
        for copy in self.saves(m):
            copy.start()

    def msg(self, m, color, phase, d, fwd):
        order, at = ORDERS[color], self.it.at
        axis = order[phase]
        idx = list(at)
        if fwd:
            idx[axis] = self.it.by[3 if d == 0 else 1][axis]
        for p in range(phase + 1, 3):
            idx[order[p]] = slice(None)
        part = piece(KIND_OF[m], color, d if fwd else None)
        dst = self.whole[m].at[(*idx, *part)]
        src = self.held(m).at[part] if phase == 2 and not fwd else dst
        return self.sets(m, phase, fwd, src, dst, (self.it.right if d == 0 else self.it.left)[axis])

    def sets(self, m, phase, fwd, src, dst, to):
        k = phase * 2 + int(fwd)
        return pltpu.make_async_remote_copy(src_ref=src, dst_ref=dst, send_sem=self.ssem.at[m, k], recv_sem=self.rsem.at[m, k],
            device_id={"dp": to}, device_id_type=MESH)

    def own_set(self, color):
        axis = ORDERS[color][0]
        idx = [slice(None)] * 3
        idx[axis] = self.it.at[axis]
        return self.whole[-1].at[(*idx, color)]

    def all(self, m, phase, fwd):
        much = self.whole[m].at[(*(0,) * phase, slice(0, 1 if fwd else 2))]
        return self.sets(m, phase, fwd, much, much, self.it.right[0])

    def send(self, m, phase, fwd):
        if fwd:
            self.all(m, phase, False).wait_recv()
        elif phase < 2:
            self.all(m, phase + 1, True).wait_recv()
        if not fwd and phase == 1:
            self.mine(m).wait()
        for color in range(3):
            for d in (0, 1):
                self.msg(m, color, phase, d, fwd).start()

    def end(self):
        for m in range(len(ORDER)):
            for copy in self.saves(m):
                copy.wait()
            last = int(m == len(ORDER) - 1)
            if not last:
                self.all(m, 0, True).wait_recv()
            for phase in range(last, 3):
                for fwd in (False, True):
                    self.all(m, phase, fwd).wait_send()


def dot(a, b, over=(1, 0)):
    return lax.dot_general(a, b, ((over[:1], over[1:]), ((), ())), preferred_element_type=F32)


WIDTH = 512
ROWS = 128
ONCE = pl.Buffered(1)
ANYWHERE = pl.BlockSpec(memory_space=pl.ANY)


def normed(h):
    wide = h.astype(F32)
    scale = lax.rsqrt(jnp.mean(wide**2, -1, keepdims=True) + 1e-6)
    return (wide * scale).astype(BF)


def normed_back(h, by_a, by_h):
    wide, by_a = h.astype(F32), by_a.astype(F32)
    scale = lax.rsqrt(jnp.mean(wide**2, -1, keepdims=True) + 1e-6)
    along = jnp.mean(by_a * wide, -1, keepdims=True)
    return (by_h.astype(F32) + (by_a * scale - wide * (along * scale**3)).astype(BF).astype(F32)).astype(BF)


def pack(out, tile):
    tile = tile.reshape(*out.shape[:-3], 8, 8, 1536)
    for c in range(3):
        for g in range(8):
            out[..., c, :, 512 * g:512 * g + 512] = tile[..., g, :, 512 * c:512 * c + 512].astype(BF)


def rows_of(ref):
    return [pl.ds(ROWS * r, ROWS) for r in range(ref.shape[0] // ROWS)]


def forward_kernel(h, y, w_gate, w_up, w_down, gate, up, act, out, by_down, a_t, by_y, a, acc, sem):
    step, tiles = pl.program_id(0), pl.num_programs(0) // 2
    late = pltpu.make_async_copy(y, by_y, sem)

    @pl.when(step == 0)
    def _():
        late.start()
        acc[...] = jnp.zeros_like(acc)
        for r in rows_of(h):
            a[r] = normed(h[r])

    @pl.when(step == tiles)
    def _():
        late.wait()
        for r in rows_of(h):
            out[r] = (h[r].astype(F32) + acc[r].astype(BF).astype(F32)).astype(BF)
            a[r] = normed(out[r])
            a_t[:, r] = a[r].T

    g, u = dot(a[...], w_gate[0]), dot(a[...], w_up[0])
    gate[0], up[0] = g, u
    hidden = (jax.nn.silu(g) * u).astype(BF)

    @pl.when(step < tiles)
    def _():
        act[...] = hidden
        acc[...] += dot(hidden, w_down[0])

    @pl.when(step >= tiles)
    def _():
        pack(by_down, dot(hidden, by_y[...], (0, 0)))


def forward(h, by_y, weights):
    (tokens, d), hidden = h.shape, weights[0].shape[2]
    tiles = hidden // WIDTH
    once = pl.BlockSpec((tokens, d), lambda i: (0, 0), pipeline_mode=ONCE)
    w_in = pl.BlockSpec((1, d, WIDTH), lambda i: (i // tiles, 0, lax.rem(i, tiles)))
    both = pl.BlockSpec((1, tokens, WIDTH), lambda i: (i // tiles, 0, lax.rem(i, tiles)))
    one, two = lambda i: lax.min(i, tiles - 1), lambda i: lax.max(i - tiles, 0)
    wide = jax.ShapeDtypeStruct((2, tokens, hidden), F32)
    return pl.pallas_call(forward_kernel, grid=(2 * tiles,), name="forward",
        in_specs=[once, ANYWHERE, w_in, w_in, pl.BlockSpec((1, WIDTH, d), lambda i: (0, one(i), 0))],
        out_specs=[both, both, pl.BlockSpec((tokens, WIDTH), lambda i: (0, one(i))), once, pl.BlockSpec((WIDTH // 64, *WIDE), lambda i: (two(i), 0, 0, 0)),
            pl.BlockSpec((d, tokens), lambda i: (0, 0), pipeline_mode=ONCE)],
        out_shape=[wide, wide, jax.ShapeDtypeStruct((tokens, hidden), BF), jax.ShapeDtypeStruct((tokens, d), BF), jax.ShapeDtypeStruct((64, *WIDE), BF),
            jax.ShapeDtypeStruct((d, tokens), BF)],
        scratch_shapes=[pltpu.VMEM((tokens, d), BF), pltpu.VMEM((tokens, d), BF), pltpu.VMEM((tokens, d), F32), pltpu.SemaphoreType.DMA],
        compiler_params=pltpu.CompilerParams(vmem_limit_bytes=VMEM))(h, by_y, *weights)


def adamw(w, m, v, g):
    m = 0.9 * m + 0.1 * g
    v = 0.95 * v + 0.05 * g * g
    step = m * lax.rsqrt(v + 1e-8) + 0.1 * w
    return (w - 0.02 * step).astype(BF), m, v


PLAN = {
    "start": {
        (0, 0): (('A', 0),),
    },
    "top": {
        (1, 0): (('B', 0),),
        (4, 1): (('F', 'c', 0, 0, 0), ('F', 'c', 0, 1, 1),),
        (5, 0): (('P', 'c', 0, 0, 0), ('F', 'c', 0, 2, 0),),
        (5, 1): (('P', 'c', 0, 1, 1),),
        (6, 0): (('P', 'c', 0, 2, 0),),
    },
    "up": {
        (0, 0): (('A', 1),),
        (1, 0): (('F', 't', 0, 0, 1),),
        (2, 0): (('P', 't', 0, 0, 1), ('F', 't', 0, 1, 0), ('B', 1),),
        (3, 0): (('P', 't', 0, 1, 0), ('F', 't', 0, 2, 1),),
        (4, 0): (('P', 't', 0, 2, 1),),
        (7, 0): (('F', 'c', 1, 0, 0), ('F', 'c', 1, 1, 1),),
    },
    "mid": {
        (0, 0): (('P', 'c', 1, 0, 0), ('F', 'c', 1, 2, 0), ('A', 2),),
        (1, 0): (('P', 'c', 1, 1, 1),),
        (2, 0): (('P', 'c', 1, 2, 0), ('O', 'c', 2, 0),),
        (6, 0): (('F', 't', 1, 0, 1), ('B', 2),),
    },
    "turn": {
        (2, 0): (('F', 't', 1, 1, 0),),
        (3, 0): (('O', 't', 2, 0),),
    },
    "down": {
        (0, 0): (('P', 't', 1, 0, 1), ('F', 't', 1, 2, 1),),
        (1, 0): (('P', 't', 1, 1, 0), ('F', 'c', 2, 0, 0),),
        (2, 0): (('P', 't', 1, 2, 1), ('O', 'c', 3, 0),),
        (3, 0): (('P', 'c', 2, 0, 0), ('F', 'c', 2, 1, 1), ('F', 'c', 2, 2, 0),),
        (4, 0): (('P', 'c', 2, 1, 1),),
        (5, 0): (('O', 'c', 2, 1), ('P', 'c', 2, 2, 0),),
        (7, 0): (('O', 't', 3, 0),),
    },
    "low": {
        (0, 0): (('A', 3),),
        (1, 1): (('F', 't', 2, 0, 1), ('F', 't', 2, 1, 0), ('B', 3),),
        (2, 0): (('O', 't', 2, 1),),
        (2, 1): (('P', 't', 2, 0, 1), ('F', 't', 2, 2, 1),),
        (3, 0): (('P', 't', 2, 1, 0),),
        (3, 1): (('P', 't', 2, 2, 1), ('F', 'c', 3, 0, 0), ('F', 'c', 3, 1, 1),),
        (4, 0): (('P', 'c', 3, 0, 0), ('F', 'c', 3, 2, 0),),
        (4, 1): (('P', 'c', 3, 1, 1),),
        (5, 0): (('P', 'c', 3, 2, 0),),
        (6, 1): (('O', 'c', 3, 1),),
        (7, 1): (('O', 'c', 2, 2),),
    },
    "last": {
        (0, 0): (('A', 4),),
        (3, 0): (('F', 't', 3, 0, 1), ('F', 't', 3, 1, 0),),
        (4, 0): (('O', 't', 3, 1), ('B', 4),),
        (6, 0): (('O', 't', 2, 2),),
        (7, 0): (('P', 't', 3, 0, 1), ('F', 't', 3, 2, 1),),
    },
}
TAIL = (
    ('P', 't', 3, 1, 0), ('P', 't', 3, 2, 1), ('F', 'c', 4, 0, 0), ('F', 'c', 4, 1, 1), ('P', 'c', 4, 0, 0), ('P', 'c', 4, 1, 1),
    ('F', 'c', 4, 2, 0), ('u', 0), ('P', 'c', 4, 2, 0), ('u', 1), ('g', 0, 2, 'o'), ('g', 1, 2, 'o'),
    ('O', 'c', 3, 2), ('O', 'c', 2, 3), ('A', 5), ('F', 't', 4, 0, 1), ('F', 't', 4, 1, 0), ('B', 5),
    ('g', 0, 2, 'f'), ('O', 't', 3, 2), ('u', 2), ('g', 1, 2, 'f'), ('g', 2, 2, 'o'), ('O', 't', 2, 3),
    ('P', 't', 4, 0, 1), ('P', 't', 4, 1, 0), ('F', 't', 4, 2, 1), ('P', 't', 4, 2, 1), ('F', 'c', 5, 0, 0), ('F', 'c', 5, 1, 1),
    ('P', 'c', 5, 0, 0), ('P', 'c', 5, 1, 1), ('F', 'c', 5, 2, 0), ('P', 'c', 5, 2, 0), ('g', 0, 1, 'o'), ('g', 1, 1, 'o'),
    ('O', 'c', 3, 3), ('g', 2, 2, 'f'), ('O', 'c', 2, 4), ('F', 't', 5, 0, 1), ('F', 't', 5, 1, 0), ('g', 0, 1, 'f'),
    ('O', 't', 3, 3), ('u', 3), ('g', 3, 2, 'o'), ('g', 1, 1, 'f'), ('g', 2, 1, 'o'), ('O', 't', 2, 4),
    ('P', 't', 5, 0, 1), ('P', 't', 5, 1, 0), ('F', 't', 5, 2, 1), ('P', 't', 5, 2, 1), ('g', 3, 2, 'f'), ('g', 0, 0, 'o'),
    ('O', 'c', 3, 4), ('g', 2, 1, 'f'), ('O', 'c', 2, 5), ('g', 3, 1, 'o'), ('O', 't', 3, 4), ('u', 4),
    ('g', 4, 2, 'o'), ('g', 0, 0, 'f'), ('O', 't', 2, 5), ('g', 3, 1, 'f'), ('g', 4, 2, 'f'), ('g', 1, 0, 'o'),
    ('O', 'c', 3, 5), ('g', 4, 1, 'o'), ('g', 2, 0, 'o'), ('O', 't', 3, 5), ('u', 5), ('g', 5, 2, 'o'),
    ('g', 4, 1, 'f'), ('g', 1, 0, 'f'), ('g', 5, 2, 'f'), ('g', 2, 0, 'f'), ('g', 5, 1, 'o'), ('g', 3, 0, 'o'),
    ('g', 5, 1, 'f'), ('g', 4, 0, 'o'), ('g', 3, 0, 'f'), ('g', 4, 0, 'f'),
)


def backward_kernel(names, by_down1, h0, h1, by_y, a_t, gates, ups, act0, *refs):
    refs = list(refs)
    pop = lambda n: [refs.pop(0) for _ in range(n)]
    weights, blocks, moments, whole, new = pop(3), pop(3), [pop(2) for _ in range(3)], pop(6), [pop(2) for _ in range(3)]
    sets = pop(3)
    by_gate1, by_up1, by_gate0, by_up0, by_down0, hid_gate, hid_up = pop(7)
    away = pop(18)
    states, turned, start_sem = pop(3)
    sems = pop(5)
    has = dict(zip(names, away + refs, strict=True))
    w_gate, w_up, w_down = weights
    it = Sums([by_down1, by_gate1, by_up1, by_down0, by_gate0, by_up0], has)
    (tokens, d), hidden = h0.shape, act0.shape[1]
    tall, wide = pl.BlockSpec((WIDTH, d), lambda i: (i, 0)), pl.BlockSpec((d, WIDTH), lambda i: (0, i))
    across = pl.BlockSpec((tokens, WIDTH), lambda i: (0, i))
    cut = pl.BlockSpec((4, 4, 4, 3, 8, WIDTH), lambda i: (0, 0, 0, 0, 0, i))
    packed = pl.BlockSpec((1, 2, 4, *WIDE), lambda i: (i // 2, lax.rem(i, 2), 0, 0, 0, 0))

    def do(op):
        if op[0] in "AB":
            it.send(*op)
        elif op[0] == "F":
            it.fetch(*op[1:])
        elif op[0] == "P":
            it.first(*op[1:])
        else:
            it.later(*op[1:])

    def loop(stage, body, ins, outs, *at):
        def hook(sub):
            for (tile, where), ops in PLAN[stage].items():
                if where == sub:
                    @pl.when(pl.program_id(0) == tile)
                    def _():
                        for op in ops:
                            do(op)

        pltpu.emit_pipeline(functools.partial(body, hook), grid=(hidden // WIDTH,), in_specs=ins, out_specs=outs)(*at)

    def into(hook, gate, up, w_down, by_gate_w, hid_up, by_gate):
        hook(0)
        for r in [pl.ds(256 * i, 256) for i in range(tokens // 256)]:
            g, u = gate[r], up[r]
            by_act = dot(states[r], w_down[...], (1, 1)).astype(BF).astype(F32)
            part = jax.nn.sigmoid(g)
            silu = g * part
            hid_up[r] = (by_act * silu).astype(BF)
            by_gate[r] = (by_act * u * (part + silu * (1 - part))).astype(BF)
        by_gate_w[...] = dot(turned[...], by_gate[...]).reshape(by_gate_w.shape).astype(BF)
        hook(1)

    def of_up(hook, by_up, by_up_w):
        hook(0)
        by_up_w[...] = dot(turned[...], by_up[...]).reshape(by_up_w.shape).astype(BF)

    def down(hook, act, by_w):
        hook(0)
        pack(by_w, dot(act[...], states[...], (0, 0)))

    def back_to_states(acc, late0, late1, late_sem):
        acc[...] = jnp.zeros_like(acc)

        def more(hook, by_gate, by_up, w_gate, w_up):
            hook(0)
            acc[...] += dot(by_gate[...], w_gate[...], (1, 1)) + dot(by_up[...], w_up[...], (1, 1))

        loop("mid", more, [across, across, wide, wide], [], hid_gate, hid_up, w_gate.at[1], w_up.at[1])
        def copies(r):
            rows, slot = pl.ds(pl.multiple_of(128 * r, 128), 128), lax.rem(r, 2)
            return [pltpu.make_async_copy(ref.at[rows], buf.at[slot], late_sem.at[slot, i]) for i, (ref, buf) in enumerate(((h0, late0), (h1, late1)))]

        for copy in copies(0):
            copy.start()

        @over(tokens // 128)
        def _(r):
            for (tile, _), ops in PLAN["turn"].items():
                @pl.when(r == 2 * tile)
                def _():
                    for op in ops:
                        do(op)

            @pl.when(r + 1 < tokens // 128)
            def _():
                for copy in copies(r + 1):
                    copy.start()

            for copy in copies(r):
                copy.wait()
            rows, slot = pl.ds(pl.multiple_of(128 * r, 128), 128), lax.rem(r, 2)
            turned[:, rows] = normed(late0[slot]).T
            states[rows] = normed_back(late1[slot], acc[rows].astype(BF), states[rows])

    def tail(aside, aside_sem, *bufs):
        last = Gather(it, blocks, moments, whole, new, dict(zip(gather_scratch(), bufs, strict=True)), sems)
        for m in range(len(ORDER)):
            for copy in last.loads(m):
                copy.start()
        for op in TAIL:
            if op[0] == "u":
                last.adamw(op[1])
            elif op[0] == "g":
                last.send(op[1], op[2], op[3] == "f")
            else:
                do(op)
        last.all(5, 1, True).wait_recv()
        into = [pltpu.make_async_copy(last.own_set(c), aside.at[c], aside_sem.at[c]) for c in range(3)]
        out = [pltpu.make_async_copy(aside.at[c], sets[c], aside_sem.at[c]) for c in range(3)]
        for copy in into:
            copy.start()
        for one, two in zip(into, out):
            one.wait()
            two.start()
        it.end(0, 5)
        last.end()
        for copy in out:
            copy.wait()

    early = [pltpu.make_async_copy(by_y, states, start_sem.at[0]), pltpu.make_async_copy(a_t, turned, start_sem.at[1])]
    for copy in early:
        copy.start()
    greet(it.left, it.right)
    for op in PLAN["start"][0, 0]:
        do(op)

    def first(hook, *tiles):
        @pl.when(pl.program_id(0) == 0)
        def _():
            for copy in early:
                copy.wait()

        into(hook, *tiles)

    loop("top", first, [across, across, tall], [cut, across, across], gates.at[1], ups.at[1], w_down.at[1], by_gate1, hid_up, hid_gate)
    loop("up", of_up, [across], [cut], hid_up, by_up1)
    pl.run_scoped(back_to_states, pltpu.VMEM((tokens, d), F32), *[pltpu.VMEM((2, 128, d), BF)] * 2, pltpu.SemaphoreType.DMA((2, 2)))
    loop("down", down, [across], [packed], act0, by_down0)
    loop("low", into, [across, across, tall], [cut, across, across], gates.at[0], ups.at[0], w_down.at[0], by_gate0, hid_up, hid_gate)
    loop("last", of_up, [across], [cut], hid_up, by_up0)
    pl.run_scoped(tail, pltpu.VMEM((3, 4, 4, 8, 4096), BF), pltpu.SemaphoreType.DMA((3,)), *gather_scratch().values())


def backward(by_down1, states, hidden_states, weights, moments, cid):
    near, away = sums_scratch(6)
    tokens, d = states[0].shape
    hidden = weights[0].shape[2]
    args = [by_down1.reshape(4, 4, 4, *WIDE), *states, *hidden_states, *weights, *(w.reshape(2, 64, *BLOCK[k]) for w, k in zip(weights, KINDS)), *(t.reshape(2, *BLOCK[k]) for pair, k in zip(moments, KINDS) for t in pair)]
    across = jax.ShapeDtypeStruct((tokens, hidden), BF)
    outs = [*(jax.ShapeDtypeStruct((4, 4, 4, *BLOCK[k]), BF) for k in KIND_OF), *(jax.ShapeDtypeStruct((2, *BLOCK[k]), F32) for k in KINDS for _ in range(2)), *[jax.ShapeDtypeStruct((4, 4, 8, 4096), BF)] * 3,
        *[jax.ShapeDtypeStruct((4, 4, 4, *WIDE), BF)] * 5, across, across, *away.values()]
    dma = pltpu.SemaphoreType.DMA
    scratch = [pltpu.VMEM((tokens, d), BF), pltpu.VMEM((d, tokens), BF), dma((2,)),
        dma((6, 3)), dma((6, 2)), dma((6,)), dma((6, 6)), dma((6, 6))]
    out = pl.pallas_call(
        functools.partial(backward_kernel, (*away, *near)),
        in_specs=[ANYWHERE] * len(args), out_specs=[ANYWHERE] * len(outs), out_shape=outs, scratch_shapes=scratch + list(near.values()),
        compiler_params=pltpu.CompilerParams(collective_id=cid, has_side_effects=True, vmem_limit_bytes=VMEM),
        name="backward",
    )(*args)
    return out[:5], [out[6 + 2 * i:8 + 2 * i] for i in range(3)], out[12:15]


AHEAD = 8


class Move:
    def __init__(self, sems):
        self.in_sem, self.out_sem = sems
        self.moves, self.used = [], {}

    def add(self, source, ring, slots, place):
        self.used[id(ring)] = slot = (self.used.get(id(ring), -1) + 1) % slots
        self.moves.append((source, ring.at[slot] if slots > 1 else ring, place, (id(ring), slot)))

    def copies(self, i):
        source, slot, place, _ = self.moves[i]
        return pltpu.make_async_copy(source, slot, self.in_sem.at[i]), pltpu.make_async_copy(slot, place, self.out_sem.at[i])

    def run(self):
        n, stored = len(self.moves), set()
        for i in range(n + AHEAD):
            if i < n:
                for j in range(i):
                    if j not in stored and self.moves[j][3] == self.moves[i][3]:
                        self.copies(j)[1].wait()
                        stored.add(j)
                self.copies(i)[0].start()
            if 0 <= i - AHEAD < n:
                into, out = self.copies(i - AHEAD)
                into.wait()
                out.start()
        for i in range(n):
            if i not in stored:
                self.copies(i)[1].wait()


def settle_kernel(*refs):
    whole, new, outs, news, rings, held, sems = refs[:5], refs[5:11], refs[11:14], refs[14:20], refs[20:22], refs[22:28], refs[28:]
    move = Move(sems)
    for (layer, i), array in zip(ORDER, whole):
        for x in range(4):
            for y in (0, 2):
                move.add(array.at[x, pl.ds(y, 2)], rings[i // 2], 2 * AHEAD, outs[i].at[layer, x, pl.ds(y, 2)])
    for source, buf, place in zip(new, held, news):
        move.add(source, buf, 1, place)
    move.run()


def settle_last_kernel(_, *refs):
    sets, came, out, ring, sems = refs[:3], refs[3:12], refs[12], refs[13], refs[14:]
    at, move = place()[0], Move(sems)
    for c in range(3):
        axis = ORDERS[c][0]
        for k in range(4):
            idx = [slice(None)] * 3
            idx[axis] = lax.rem(at[axis] + 4 - k, 4)
            move.add(came[3 * c + k - 1] if k else sets[c], ring, 2 * AHEAD, out.at[(0, *idx, c)])
    move.run()


def settle(whole, new, sets):
    came = []
    for c in range(3):
        stride = STRIDE[ORDERS[c][0]]
        for k in (2, 1, 3):
            ring = [(i, i + ((i // stride + k) % 4 - i // stride % 4) * stride) for i in range(64)]
            came.append((3 * c + k - 1, lax.ppermute(sets[c], "dp", ring)))
    flat = [t for pair in new for t in pair]
    dma = pltpu.SemaphoreType.DMA
    both = {k: jax.ShapeDtypeStruct((2, 4, 4, 4, *BLOCK[k]), BF) for k in ("wide", "tall")}
    ring = {k: pltpu.VMEM((2 * AHEAD, 2, 4, *BLOCK[k]), BF) for k in ("wide", "tall")}
    call = functools.partial(pl.pallas_call, compiler_params=pltpu.CompilerParams(vmem_limit_bytes=VMEM),
        cost_estimate=pl.CostEstimate(flops=60000000000, bytes_accessed=130000000, transcendentals=0))
    gate, up, down, *flat = call(settle_kernel, in_specs=[ANYWHERE] * 11, out_specs=[ANYWHERE] * 9,
        out_shape=[both["wide"], both["wide"], both["tall"], *(jax.ShapeDtypeStruct(t.shape, t.dtype) for t in flat)],
        scratch_shapes=[ring["wide"], ring["tall"], *(pltpu.VMEM(t.shape, t.dtype) for t in flat), dma((46,)), dma((46,))], name="settle",
    )(*whole, *flat)
    up = call(settle_last_kernel, in_specs=[ANYWHERE] * 13, out_specs=ANYWHERE, out_shape=both["wide"], input_output_aliases={0: 0},
        scratch_shapes=[pltpu.VMEM((2 * AHEAD, 4, 4, 8, 4096), BF), dma((12,)), dma((12,))], name="settle_last",
    )(up, *sets, *(t for _, t in sorted(came, key=lambda one: one[0])))
    return [gate, up, down], [flat[2 * i:2 * i + 2] for i in range(3)]


def solution(mesh):
    def step(x, dy, *arrays):
        weights, m, v = (arrays[i : i + 3] for i in (0, 3, 6))
        layers = weights[0].shape[0]
        assert layers == 2
        h0, by_y = x[0], dy[0]
        gates, ups, act0, h1, by_down1, a_t = forward(h0, by_y, weights)
        whole, new, sets = backward(by_down1, [h0, h1, by_y, a_t], [gates, ups, act0], weights, list(zip(m, v)), 1)
        out, new = settle(whole, new, sets)
        out = [t.reshape(w.shape) for t, w in zip(out, weights)]
        new = [[t.reshape(a.shape) for t in pair] for pair, a in zip(new, m)]
        return (*out, *(new[i][which] for which in (0, 1) for i in range(3)))

    blocks = P(None, "dp", None)
    return jax.shard_map(step, mesh=mesh, in_specs=(P(("rep", "dp")),) * 2 + (P(),) * 3 + (blocks,) * 6,
        out_specs=(P("rep"),) * 3 + (P("rep", "dp", None),) * 6, check_vma=False)
```
